8 devices in a mesh: sys: 1 (over z), zdom: 2 (over y), ydom: 4 (over x, core).
Axes of the slice: x: 2, y: 2, z: 1, core: 2. Of those that a mesh axis runs over, the one named last changes fastest.
Arguments:
- charge: float32 [65536], P(('sys', 'ydom', 'zdom'))
- real_mask: int32 [65536], P(('sys', 'ydom', 'zdom'))
- grid_idx: int32 [65536, 3], P(('sys', 'ydom', 'zdom'))
- spline_w: float32 [65536, 3, 4], P(('sys', 'ydom', 'zdom'))
- influence: float32 [128, 128, 128], P(('sys', 'ydom'), 'zdom')
Outputs:
- output 1: float32 [128, 128, 128], P(('sys', 'ydom'), 'zdom')
- output 2: float32 [1], P('sys')
All inputs are finite; a program needn't handle non-finite values.
Results may differ from the reference program's by a relative error of at most 0.001.
Values are sent between devices in bfloat16 or wider.
A program may use at most 1 GiB of HBM per device.

```python
import jax
import jax.numpy as jnp
from jax import lax

GRID_SIDE = 128
PER_DEV = 8192
Y_DEVS = 4
Z_DEVS = 2


def bspline_weights(frac_part):
    frac_sq = frac_part * frac_part
    frac_cube = frac_sq * frac_part
    w_zero = (1.0 - frac_part) * (1.0 - frac_part) * (1.0 - frac_part) / 6.0
    w_one = (3.0 * frac_cube - 6.0 * frac_sq + 4.0) / 6.0
    w_two = (-3.0 * frac_cube + 3.0 * frac_sq + 3.0 * frac_part + 1.0) / 6.0
    w_three = frac_cube / 6.0
    return jnp.stack([w_zero, w_one, w_two, w_three], axis=-1)


def edge_index(key, count, length):
    key_near, key_edge, key_any = jax.random.split(key, 3)
    near_edge = jax.random.randint(key_near, (count,), 0, 2)
    at_edge = length - 3 + jax.random.randint(key_edge, (count,), 0, 3)
    anywhere = jax.random.randint(key_any, (count,), 0, length)
    return jnp.where(near_edge == 1, at_edge, anywhere)


def setup_inputs(seed: int = 0, part: int = 0) -> dict:
    dev_count = Y_DEVS * Z_DEVS
    slot_count = dev_count * PER_DEV
    len_y = GRID_SIDE // Y_DEVS
    len_z = GRID_SIDE // Z_DEVS
    sub_keys = jax.random.split(jax.random.fold_in(jax.random.key(seed), part), 8)
    real_count = jax.random.randint(sub_keys[0], (dev_count, 1), PER_DEV // 8, PER_DEV + 1)
    slot_rank = jax.random.randint(sub_keys[1], (dev_count, PER_DEV), 0, PER_DEV)
    real_mask = (slot_rank < real_count).astype(jnp.int32).reshape(slot_count)
    x_idx = jax.random.randint(sub_keys[2], (slot_count,), 0, GRID_SIDE)
    y_idx = edge_index(sub_keys[3], slot_count, len_y)
    z_idx = edge_index(sub_keys[4], slot_count, len_z)
    grid_idx = jnp.stack([x_idx, y_idx, z_idx], axis=1).astype(jnp.int32)
    charge = jax.random.normal(sub_keys[5], (slot_count,), jnp.float32)
    frac_part = jax.random.uniform(sub_keys[6], (slot_count, 3), jnp.float32)
    spline_w = bspline_weights(frac_part).astype(jnp.float32)
    influence = jax.random.uniform(sub_keys[7], (GRID_SIDE, GRID_SIDE, GRID_SIDE), jnp.float32, 0.5, 1.5) * (20.0 / slot_count)
    return {'charge': charge, 'real_mask': real_mask, 'grid_idx': grid_idx, 'spline_w': spline_w, 'influence': influence}


def reference(charge, real_mask, grid_idx, spline_w, influence):
    slot_count = Y_DEVS * Z_DEVS * PER_DEV
    len_y = GRID_SIDE // Y_DEVS
    len_z = GRID_SIDE // Z_DEVS
    device = jnp.arange(slot_count) // PER_DEV
    base_x = grid_idx[:, 0]
    base_y = grid_idx[:, 1] + (device // Z_DEVS) * len_y
    base_z = grid_idx[:, 2] + (device % Z_DEVS) * len_z
    weight = charge * real_mask.astype(charge.dtype)

    def add_tap(flat_grid, tap_id):
        off_x = tap_id // 16
        off_y = (tap_id // 4) % 4
        off_z = tap_id % 4
        pos_x = (base_x + off_x) % GRID_SIDE
        pos_y = (base_y + off_y) % GRID_SIDE
        pos_z = (base_z + off_z) % GRID_SIDE
        tap_value = weight * spline_w[:, 0, off_x] * spline_w[:, 1, off_y] * spline_w[:, 2, off_z]
        flat_idx = (pos_x * GRID_SIDE + pos_y) * GRID_SIDE + pos_z
        return flat_grid.at[flat_idx].add(tap_value), None

    flat_grid = lax.scan(add_tap, jnp.zeros((GRID_SIDE * GRID_SIDE * GRID_SIDE,), charge.dtype), jnp.arange(64))[0]
    charge_grid = flat_grid.reshape(GRID_SIDE, GRID_SIDE, GRID_SIDE)
    spectrum = jnp.fft.fftn(charge_grid)
    mode_energy = 0.5 * influence * (spectrum.real * spectrum.real + spectrum.imag * spectrum.imag)
    energy = jnp.sum(mode_energy) / (GRID_SIDE * GRID_SIDE * GRID_SIDE)
    return mode_energy, jnp.reshape(energy, (1,))
```

```python
import functools
import math
import numpy as np
import jax
import jax.numpy as jnp
from jax import lax
from jax.experimental import pallas as pl
from jax.experimental.pallas import tpu as pltpu
from jax.sharding import PartitionSpec as P

MESH = pl.DeviceIdType.MESH
F32 = jnp.float32
BF16 = jnp.bfloat16
GRID = 128
LEN_Y = 32
LEN_Z = 64
GHOST = 3
BLOCK = 256
Y_ROWS = 40
GROUPS = 4
CHUNKS = 4
NT = (((1,), (1,)), ((), ()))
NN = (((1,), (0,)), ((), ()))


def split_table(table):
    table = np.asarray(table, np.float32)
    high = table.astype(jnp.bfloat16)
    low = (table - high.astype(np.float32)).astype(jnp.bfloat16)
    return np.stack([high, low])


def dft_tables():
    k = np.arange(GRID)
    phase = 2.0 * np.pi * ((k[:, None] * k[None, :]) % GRID) / GRID
    cos, sin = np.cos(phase), np.sin(phase)
    x_table = np.concatenate([cos, -sin], axis=0)
    z_table = []
    for half in range(2):
        c = cos[64 * half:64 * half + 64]
        s = sin[64 * half:64 * half + 64]
        z_table.append(np.block([[c, -s], [s, c]]))
    return split_table(x_table), split_table(np.stack(z_table))


def split(value):
    high = value.astype(BF16)
    low = (value - high.astype(F32)).astype(BF16)
    return high, low


def dot(a, b, dims):
    return lax.dot_general(a, b, dims, preferred_element_type=F32)


def taps(base, weights, rows):
    delta = lax.broadcasted_iota(jnp.int32, (rows, base.shape[1]), 0) - base
    out = jnp.where(delta == 3, weights[3:4], 0.0)
    for s in (2, 1, 0):
        out = jnp.where(delta == s, weights[s:s + 1], out)
    return out


def c_add(a, b):
    return a[0] + b[0], a[1] + b[1]


def c_sub(a, b):
    return a[0] - b[0], a[1] - b[1]


def c_mul(a, turn):
    turn = turn % 1.0
    if turn == 0.0:
        return a
    if turn == 0.25:
        return a[1], -a[0]
    if turn == 0.5:
        return -a[0], -a[1]
    if turn == 0.75:
        return -a[1], a[0]
    c, s = math.cos(2 * math.pi * turn), math.sin(2 * math.pi * turn)
    if turn == 0.125:
        return c * (a[0] + a[1]), c * (a[1] - a[0])
    return c * a[0] + s * a[1], c * a[1] - s * a[0]


def fft(values):
    n = len(values)
    if n == 1:
        return values
    even, odd = fft(values[0::2]), fft(values[1::2])
    turned = [c_mul(o, k / n) for k, o in enumerate(odd)]
    return [c_add(e, t) for e, t in zip(even, turned)] + [c_sub(e, t) for e, t in zip(even, turned)]


def kernel(blocks, charge, mask, index, spline, influence, x_table, z_table,
           energy_out, total_out,
           xcat, yline, zline, acc, yghost, zghost, yface, zface, corner,
           fsend, grecv, mid, hbuf, hrecv, evec, erecv,
           ghost_send, ghost_recv, a_send, a_recv, b_send, b_recv, e_send, e_recv):
    i = lax.axis_index('ydom')
    j = lax.axis_index('zdom')
    me = j * 4 + i
    i_next = lax.rem(i + 1, 4)
    j_next = 1 - j

    barrier = pltpu.get_barrier_semaphore()
    for off in range(1, 8):
        peer = lax.rem(me + off, 8)
        pl.semaphore_signal(barrier, inc=1, device_id=(0, peer // 4, lax.rem(peer, 4)), device_id_type=MESH)

    acc[...] = jnp.zeros_like(acc)
    yghost[...] = jnp.zeros_like(yghost)
    zghost[...] = jnp.zeros_like(zghost)

    def prepare(b, carry):
        lanes = pl.ds(pl.multiple_of(b * BLOCK, BLOCK), BLOCK)
        weight = charge[:, lanes] * mask[:, lanes].astype(F32)
        wx = spline[0, :, lanes] * weight
        base = index[0:1, lanes]
        delta = (lax.broadcasted_iota(jnp.int32, (GRID, BLOCK), 0) - base) & (GRID - 1)
        line = jnp.where(delta == 3, wx[3:4], 0.0)
        for s in (2, 1, 0):
            line = jnp.where(delta == s, wx[s:s + 1], line)
        high, low = split(line)
        xcat[b, 0:GRID] = high
        xcat[b, GRID:2 * GRID] = low
        yl = taps(index[1:2, lanes], spline[1, :, lanes], Y_ROWS)
        yline[b] = yl
        zl = taps(index[2:3, lanes], spline[2, :, lanes], LEN_Z + 8)
        zline[b] = zl[0:LEN_Z]
        rows = [yl[LEN_Y + t:LEN_Y + t + 1] * zl[0:LEN_Z] for t in range(GHOST)]
        rows += [zl[LEN_Z + u:LEN_Z + u + 1] * yl for u in range(GHOST)]
        rows += [jnp.zeros((8, BLOCK), F32)]
        high, low = split(jnp.concatenate(rows, axis=0))
        part = dot(high, xcat[b], NT)
        part = part[:, 0:GRID] + part[:, GRID:] + dot(low, xcat[b, 0:GRID], NT)
        yghost[...] += part[0:GHOST * LEN_Z].reshape(GHOST, LEN_Z, GRID)
        zghost[...] += part[GHOST * LEN_Z:GHOST * LEN_Z + GHOST * Y_ROWS].reshape(GHOST, Y_ROWS, GRID)
        return carry

    lax.fori_loop(0, blocks, prepare, 0)

    pl.semaphore_wait(barrier, 7)
    ghosts = []
    for n, (src, dst, peer) in enumerate([
            (yghost, yface, (0, j, i_next)),
            (zghost.at[:, 0:LEN_Y], zface, (0, j_next, i)),
            (zghost.at[:, LEN_Y:Y_ROWS], corner, (0, j_next, i_next))]):
        copy = pltpu.make_async_remote_copy(
            src_ref=src, dst_ref=dst, send_sem=ghost_send.at[n], recv_sem=ghost_recv.at[n],
            device_id=peer, device_id_type=MESH)
        copy.start()
        ghosts.append(copy)

    def spread_rows(group):
        def body(b, carry):
            zl = zline[b]
            yl = yline[b, 8 * group:8 * group + 8]
            xb = xcat[b]
            high, low = split(jnp.concatenate([yl[t:t + 1] * zl for t in range(8)], axis=0))
            part = dot(high, xb, NT)
            acc[...] += part[:, 0:GRID] + part[:, GRID:] + dot(low, xb[0:GRID], NT)
            return carry
        lax.fori_loop(0, blocks, body, 0)

    a_copies = {}
    order = list(range(GROUPS - 1, -1, -1))
    for turn, group in enumerate(order):
        if turn > 0:
            acc[...] = jnp.zeros_like(acc)
        spread_rows(group)
        if turn == 0:
            for copy in ghosts:
                copy.wait_recv()
        if group == 0:
            for t in range(GHOST):
                face = jnp.concatenate(
                    [yface[t, 0:8] + jnp.concatenate(
                        [corner[u, t:t + 1] for u in range(GHOST)] + [jnp.zeros((8 - GHOST, GRID), F32)], axis=0),
                     yface[t, 8:LEN_Z]], axis=0)
                acc[LEN_Z * t:LEN_Z * t + LEN_Z] += face
        for u in range(GHOST):
            acc[pl.ds(u, 8, stride=LEN_Z)] += zface[u, 8 * group:8 * group + 8]
        for pair in range(4):
            high, low = split(acc[128 * pair:128 * pair + 128])
            modes = dot(x_table[0], high, NT) + dot(x_table[1], high, NT) + dot(x_table[0], low, NT)
            fsend[group, 0, pair] = modes[0:GRID]
            fsend[group, 1, pair] = modes[GRID:]
        for chunk in range(CHUNKS):
            for d in (2, 1, 3):
                peer = lax.rem(i + d, 4)
                copy = pltpu.make_async_remote_copy(
                    src_ref=fsend.at[group, :, :, pl.ds(pl.multiple_of(32 * peer + 8 * chunk, 8), 8), :],
                    dst_ref=grecv.at[i, group, chunk],
                    send_sem=a_send.at[group, chunk, d], recv_sem=a_recv.at[group, chunk, d],
                    device_id=(0, j, peer), device_id_type=MESH)
                copy.start()
                a_copies[group, chunk, d] = copy
            grecv[i, group, chunk] = fsend[group, :, :, pl.ds(pl.multiple_of(32 * i + 8 * chunk, 8), 8), :]

    low_half = lax.broadcasted_iota(jnp.int32, (8, GRID), 1) < 64
    b_copies = []
    for chunk in range(CHUNKS):
        for group in range(GROUPS):
            for d in (1, 2, 3):
                a_copies[group, chunk, d].wait_recv()
        for b in range(8):
            values = []
            for a in range(8):
                q = 8 * a + b
                src, group, pair = q // 16, (q % 16) // 4, q % 4
                values.append((grecv[src, group, chunk, 0, pair], grecv[src, group, chunk, 1, pair]))
            for c, value in enumerate(fft(values)):
                value = c_mul(value, b * c / 64)
                mid[c, b, 0] = value[0]
                mid[c, b, 1] = value[1]
        for c in range(8):
            values = fft([(mid[c, b, 0], mid[c, b, 1]) for b in range(8)])
            for d, value in enumerate(values):
                k = c + 8 * d
                turned = c_mul(value, k / 128)
                left = jnp.where(low_half, value[0], pltpu.roll(value[1], 64, 1))
                right = jnp.where(low_half, pltpu.roll(turned[0], 64, 1), turned[1])
                hbuf[chunk, 0, k] = left + right
                hbuf[chunk, 1, k] = left - right
        copy = pltpu.make_async_remote_copy(
            src_ref=hbuf.at[chunk, j_next], dst_ref=hrecv.at[chunk],
            send_sem=b_send.at[chunk], recv_sem=b_recv.at[chunk],
            device_id=(0, j_next, i), device_id_type=MESH)
        copy.start()
        b_copies.append(copy)

    table = [jnp.concatenate([z_table[n, j], z_table[n, j_next]], axis=0) for n in range(2)]
    total = jnp.zeros((8, GRID), F32)
    for chunk in range(CHUNKS):
        b_copies[chunk].wait_recv()
        rows = jnp.concatenate([hbuf[chunk, j].reshape(512, GRID), hrecv[chunk].reshape(512, GRID)], axis=1)
        high, low = split(rows)
        modes = dot(high, table[0], NN) + dot(high, table[1], NN) + dot(low, table[0], NN)
        re, im = modes[:, 0:GRID], modes[:, GRID:]
        power = jnp.transpose((re * re + im * im).reshape(64, 8, GRID), (1, 0, 2))
        mode = 0.5 * influence[8 * chunk:8 * chunk + 8] * power
        energy_out[8 * chunk:8 * chunk + 8] = mode
        total = total + jnp.sum(mode.reshape(64, 8, GRID), axis=0)

    evec[...] = total
    e_copies = []
    for off in range(1, 8):
        peer = lax.rem(me + off, 8)
        copy = pltpu.make_async_remote_copy(
            src_ref=evec, dst_ref=erecv.at[me], send_sem=e_send.at[off], recv_sem=e_recv.at[off],
            device_id=(0, peer // 4, lax.rem(peer, 4)), device_id_type=MESH)
        copy.start()
        e_copies.append(copy)
    erecv[me] = total
    for copy in e_copies:
        copy.wait_recv()
    grand = erecv[0]
    for n in range(1, 8):
        grand = grand + erecv[n]
    total_out[0] = jnp.sum(grand) * (1.0 / (GRID * GRID * GRID))

    for copy in ghosts + list(a_copies.values()) + b_copies + e_copies:
        copy.wait_send()


def solution(mesh):
    slot_spec = P(('sys', 'ydom', 'zdom'))
    mode_spec = P(('sys', 'ydom'), 'zdom', None)
    x_table, z_table = dft_tables()

    def local_energy(charge, real_mask, grid_idx, spline_w, influence):
        slots = charge.shape[0]
        blocks = slots // BLOCK
        vmem = pl.BlockSpec(memory_space=pltpu.VMEM)
        mode_energy, energy = pl.pallas_call(
            functools.partial(kernel, blocks),
            name='pme',
            out_shape=(jax.ShapeDtypeStruct(influence.shape, F32), jax.ShapeDtypeStruct((1,), F32)),
            in_specs=[vmem] * 7,
            out_specs=(vmem, pl.BlockSpec(memory_space=pltpu.SMEM)),
            scratch_shapes=[
                pltpu.VMEM((blocks, 2 * GRID, BLOCK), BF16),
                pltpu.VMEM((blocks, Y_ROWS, BLOCK), F32),
                pltpu.VMEM((blocks, LEN_Z, BLOCK), F32),
                pltpu.VMEM((8 * LEN_Z, GRID), F32),
                pltpu.VMEM((GHOST, LEN_Z, GRID), F32),
                pltpu.VMEM((GHOST, Y_ROWS, GRID), F32),
                pltpu.VMEM((GHOST, LEN_Z, GRID), F32),
                pltpu.VMEM((GHOST, LEN_Y, GRID), F32),
                pltpu.VMEM((GHOST, 8, GRID), F32),
                pltpu.VMEM((GROUPS, 2, 4, GRID, GRID), F32),
                pltpu.VMEM((4, GROUPS, CHUNKS, 2, 4, 8, GRID), F32),
                pltpu.VMEM((8, 8, 2, 8, GRID), F32),
                pltpu.VMEM((CHUNKS, 2, 64, 8, GRID), F32),
                pltpu.VMEM((CHUNKS, 64, 8, GRID), F32),
                pltpu.VMEM((8, GRID), F32),
                pltpu.VMEM((8, 8, GRID), F32),
                pltpu.SemaphoreType.DMA((3,)),
                pltpu.SemaphoreType.DMA((3,)),
                pltpu.SemaphoreType.DMA((GROUPS, CHUNKS, 4)),
                pltpu.SemaphoreType.DMA((GROUPS, CHUNKS, 4)),
                pltpu.SemaphoreType.DMA((CHUNKS,)),
                pltpu.SemaphoreType.DMA((CHUNKS,)),
                pltpu.SemaphoreType.DMA((8,)),
                pltpu.SemaphoreType.DMA((8,)),
            ],
            compiler_params=pltpu.CompilerParams(collective_id=0, has_side_effects=True, vmem_limit_bytes=56 * 1024 * 1024),
        )(charge.reshape(1, slots), real_mask.reshape(1, slots), grid_idx.T,
          jnp.transpose(spline_w, (1, 2, 0)), influence, jnp.asarray(x_table), jnp.asarray(z_table))
        return mode_energy, energy

    return jax.shard_map(local_energy, mesh=mesh, in_specs=(slot_spec, slot_spec, P(('sys', 'ydom', 'zdom'), None), P(('sys', 'ydom', 'zdom'), None, None), mode_spec), out_specs=(mode_spec, P('sys')), check_vma=False)
```

```python
import functools
import math
import numpy as np
import jax
import jax.numpy as jnp
from jax import lax
from jax.experimental import pallas as pl
from jax.experimental.pallas import tpu as pltpu
from jax.sharding import PartitionSpec as P

MESH = pl.DeviceIdType.MESH
F32 = jnp.float32
BF16 = jnp.bfloat16
GRID = 128
LEN_Y = 32
LEN_Z = 64
GHOST = 3
BLOCK = 256
Y_ROWS = 40
CHUNKS = 4
UNROLL = 4
VMEM_LIMIT = 28 * 1024 * 1024
GROUP_B = ((2, 3), (4, 5), (0, 1), (6,), (7,))
PAIRS = tuple(tuple(bs) + tuple(8 + b for b in bs) for bs in GROUP_B)
OFFSET = tuple(sum(4 * len(p) + 1 for p in PAIRS[:g]) for g in range(len(PAIRS)))
TILES = sum(4 * len(p) + 1 for p in PAIRS)
PLACE = {pair: (g, OFFSET[g] + 4 * n) for g, pairs in enumerate(PAIRS) for n, pair in enumerate(pairs)}
NT = (((1,), (1,)), ((), ()))
NN = (((1,), (0,)), ((), ()))


def split_table(table):
    table = np.asarray(table, np.float32)
    high = table.astype(jnp.bfloat16)
    low = (table - high.astype(np.float32)).astype(jnp.bfloat16)
    return np.stack([high, low])


def dft_tables():
    k = np.arange(GRID)
    phase = 2.0 * np.pi * ((k[:, None] * k[None, :]) % GRID) / GRID
    cos, sin = np.cos(phase), np.sin(phase)
    x_table = np.concatenate([cos, -sin], axis=0)
    z_table = []
    for half in range(2):
        c = cos[64 * half:64 * half + 64]
        s = sin[64 * half:64 * half + 64]
        z_table.append(np.block([[c, -s], [s, c]]))
    return split_table(x_table), split_table(np.concatenate(z_table, axis=0))


def split(value):
    high = value.astype(BF16)
    low = (value - high.astype(F32)).astype(BF16)
    return high, low


def dot(a, b, dims):
    return lax.dot_general(a, b, dims, preferred_element_type=F32)


def taps(base, weights, rows):
    delta = lax.broadcasted_iota(jnp.int32, (rows, base.shape[1]), 0) - base
    out = jnp.where(delta == 3, weights[3:4], 0.0)
    for s in (2, 1, 0):
        out = jnp.where(delta == s, weights[s:s + 1], out)
    return out


def c_add(a, b):
    return a[0] + b[0], a[1] + b[1]


def c_sub(a, b):
    return a[0] - b[0], a[1] - b[1]


def c_mul(a, turn):
    turn = turn % 1.0
    if turn == 0.0:
        return a
    if turn == 0.25:
        return a[1], -a[0]
    if turn == 0.5:
        return -a[0], -a[1]
    if turn == 0.75:
        return -a[1], a[0]
    c, s = math.cos(2 * math.pi * turn), math.sin(2 * math.pi * turn)
    if turn == 0.125:
        return c * (a[0] + a[1]), c * (a[1] - a[0])
    return c * a[0] + s * a[1], c * a[1] - s * a[0]


def fft(values):
    n = len(values)
    if n == 1:
        return values
    even, odd = fft(values[0::2]), fft(values[1::2])
    turned = [c_mul(o, k / n) for k, o in enumerate(odd)]
    return [c_add(e, t) for e, t in zip(even, turned)] + [c_sub(e, t) for e, t in zip(even, turned)]


def kernel(blocks, charge, mask, index, spline, influence_hbm, x_table_hbm, z_table_hbm,
           energy_hbm, total_out,
           influence, x_table, z_table, energy,
           xcat, yline, zline, acc, yghost, zghost, yface, zface, corner,
           modes, fsend, grecv, scale, mid, hbuf, evec, erecv,
           load_sem, store_sem, ghost_send, ghost_recv, a_send, a_recv, e_send, e_recv):
    i = lax.axis_index('ydom')
    j = lax.axis_index('zdom')
    me = j * 4 + i
    i_next = lax.rem(i + 1, 4)
    j_next = 1 - j

    barrier = pltpu.get_barrier_semaphore()
    for off in range(1, 8):
        peer = lax.rem(me + off, 8)
        pl.semaphore_signal(barrier, inc=1, device_id=(0, peer // 4, lax.rem(peer, 4)), device_id_type=MESH)

    loads = [pltpu.make_async_copy(src, dst, load_sem.at[n]) for n, (src, dst) in enumerate(
        [(x_table_hbm, x_table), (z_table_hbm, z_table), (influence_hbm, influence)])]
    for copy in loads:
        copy.start()

    yghost[...] = jnp.zeros_like(yghost)
    zghost[...] = jnp.zeros_like(zghost)
    zface[GHOST * LEN_Y:] = jnp.zeros((5 * LEN_Y, GRID), F32)
    corner[GHOST * 8:] = jnp.zeros((5 * 8, GRID), F32)

    def prepare(step, carry):
        total = None
        for n in range(2):
            b = 2 * step + n
            lanes = pl.ds(pl.multiple_of(b * BLOCK, BLOCK), BLOCK)
            weight = charge[:, lanes] * mask[:, lanes].astype(F32)
            wx = spline[0, :, lanes] * weight
            delta = (lax.broadcasted_iota(jnp.int32, (GRID, BLOCK), 0) - index[0:1, lanes]) & (GRID - 1)
            line = jnp.where(delta == 3, wx[3:4], 0.0)
            for s in (2, 1, 0):
                line = jnp.where(delta == s, wx[s:s + 1], line)
            xhigh, xlow = split(line)
            xcat[b, 0:GRID] = xhigh
            xcat[b, GRID:2 * GRID] = xlow
            yl = taps(index[1:2, lanes], spline[1, :, lanes], Y_ROWS)
            yline[b] = yl
            zl = taps(index[2:3, lanes], spline[2, :, lanes], LEN_Z + 8)
            zline[b] = zl[0:LEN_Z]
            rows = [yl[LEN_Y + t:LEN_Y + t + 1] * zl[0:LEN_Z] for t in range(GHOST)]
            rows += [zl[LEN_Z + u:LEN_Z + u + 1] * yl for u in range(GHOST)]
            rows += [jnp.zeros((8, BLOCK), F32)]
            high, low = split(jnp.concatenate(rows, axis=0))
            both = dot(high, jnp.concatenate([xhigh, xlow], axis=0), NT)
            part = both[:, 0:GRID] + both[:, GRID:] + dot(low, xhigh, NT)
            total = part if total is None else total + part
        yghost[...] += total[0:GHOST * LEN_Z].reshape(GHOST, LEN_Z, GRID)
        zghost[...] += total[GHOST * LEN_Z:GHOST * LEN_Z + GHOST * Y_ROWS].reshape(GHOST, Y_ROWS, GRID)
        return carry

    lax.fori_loop(0, blocks // 2, prepare, 0)

    pl.semaphore_wait(barrier, 7)
    ghosts = []
    for n, (src, dst, peer) in enumerate(
            [(yghost, yface, (0, j, i_next))]
            + [(zghost.at[u, 0:LEN_Y], zface.at[LEN_Y * u:LEN_Y * u + LEN_Y], (0, j_next, i)) for u in range(GHOST)]
            + [(zghost.at[u, LEN_Y:Y_ROWS], corner.at[8 * u:8 * u + 8], (0, j_next, i_next)) for u in range(GHOST)]):
        copy = pltpu.make_async_remote_copy(
            src_ref=src, dst_ref=dst, send_sem=ghost_send.at[n], recv_sem=ghost_recv.at[n],
            device_id=peer, device_id_type=MESH)
        copy.start()
        ghosts.append(copy)

    def spread_rows(pairs):
        count = 2 * LEN_Z * len(pairs)
        acc[0:count] = jnp.zeros((count, GRID), F32)

        def body(step, carry):
            both, single = None, None
            for n in range(UNROLL):
                b = UNROLL * step + n
                zl = zline[b]
                high, low = split(jnp.concatenate(
                    [yline[b, 2 * pair + h:2 * pair + h + 1] * zl for pair in pairs for h in range(2)], axis=0))
                one, two = dot(high, xcat[b], NT), dot(low, xcat[b, 0:GRID], NT)
                both, single = (one, two) if both is None else (both + one, single + two)
            acc[0:count] += both[:, 0:GRID] + both[:, GRID:] + single
            return carry
        lax.fori_loop(0, blocks // UNROLL, body, 0)

    a_copies = []
    for group, pairs in enumerate(PAIRS):
        spread_rows(pairs)
        if group == 0:
            for copy in ghosts:
                copy.wait_recv()
            loads[0].wait()
        for n, pair in enumerate(pairs):
            for h in range(2):
                y, row = 2 * pair + h, 64 * (2 * n + h)
                if y < GHOST:
                    acc[row:row + LEN_Z] += yface[y]
                    acc[row:row + 8] += corner[pl.ds(y, 8, stride=8)]
                acc[row:row + 8] += zface[pl.ds(y, 8, stride=LEN_Y)]
        for n in range(len(pairs)):
            high, low = split(acc[128 * n:128 * n + 128])
            modes[n] = dot(x_table[0], high, NT) + dot(x_table[1], high, NT) + dot(x_table[0], low, NT)
        first, last = OFFSET[group], OFFSET[group] + 4 * len(pairs)
        for peer in range(4):
            at = [(n, c, 32 * peer + 8 * c) for n in range(len(pairs)) for c in range(CHUNKS)]
            top = jnp.full((8, GRID), 1e-30, F32)
            for n, c, row in at:
                top = jnp.maximum(top, jnp.maximum(jnp.abs(modes[n, row:row + 8]), jnp.abs(modes[n, GRID + row:GRID + row + 8])))
            code = jnp.ceil(jnp.log(top) * 1024.0)
            inverse = 32760.0 / jnp.exp(code * (1.0 / 1024.0))
            for n, c, row in at:
                re = jnp.round(modes[n, row:row + 8] * inverse).astype(jnp.int32)
                im = jnp.round(modes[n, GRID + row:GRID + row + 8] * inverse).astype(jnp.int32)
                fsend[peer, first + 4 * n + c] = (im << 16) | (re & 0xffff)
            fsend[peer, last] = code.astype(jnp.int32)
        copies = []
        for d, dj in ((2, 1), (2, 0), (1, 1), (3, 1), (1, 0), (3, 0), (0, 1)):
            peer, peer_j = lax.rem(i + d, 4), (j_next if dj else j)
            copy = pltpu.make_async_remote_copy(
                src_ref=fsend.at[peer, first:last + 1], dst_ref=grecv.at[me, first:last + 1],
                send_sem=a_send.at[group, 2 * d + dj], recv_sem=a_recv.at[group, 2 * d + dj],
                device_id=(0, peer_j, peer), device_id_type=MESH)
            copy.start()
            copies.append(copy)
        a_copies.append(copies)
        grecv[me, first:last + 1] = fsend[i, first:last + 1]

    for group, bs in enumerate(GROUP_B):
        for copy in a_copies[group]:
            copy.wait_recv()
        last = OFFSET[group] + 4 * len(PAIRS[group])
        for src in range(8):
            scale[src, group] = jnp.exp(grecv[src, last].astype(F32) * (1.0 / 1024.0)) * (1.0 / 32760.0)

        def first_stage(part, carry):
            half, chunk = part // CHUNKS, lax.rem(part, CHUNKS)
            for b in bs:
                values = []
                for a in range(8):
                    src = 4 * half + a // 2
                    word = grecv[src, PLACE[8 * (a % 2) + b][1] + chunk]
                    unit = scale[src, group]
                    values.append((((word << 16) >> 16).astype(F32) * unit, (word >> 16).astype(F32) * unit))
                for c, value in enumerate(fft(values)):
                    value = c_mul(value, b * c / 64)
                    mid[part, c, b, 0] = value[0]
                    mid[part, c, b, 1] = value[1]
            return carry
        lax.fori_loop(0, 2 * CHUNKS, first_stage, 0)

    low_half = lax.broadcasted_iota(jnp.int32, (8, GRID), 1) < 64
    sign = (1 - 2 * j).astype(F32)
    loads[1].wait()
    loads[2].wait()

    def modes_of(chunk, total):
        for half in range(2):
            for c in range(8):
                values = fft([(mid[CHUNKS * half + chunk, c, b, 0], mid[CHUNKS * half + chunk, c, b, 1]) for b in range(8)])
                for d, value in enumerate(values):
                    k = c + 8 * d
                    turned = c_mul(value, k / 128)
                    left = jnp.where(low_half, value[0], pltpu.roll(value[1], 64, 1))
                    right = jnp.where(low_half, pltpu.roll(turned[0], 64, 1), turned[1])
                    hbuf[half, k] = left + sign * right
        rows = jnp.concatenate([hbuf[0].reshape(512, GRID), hbuf[1].reshape(512, GRID)], axis=1)
        high, low = split(rows)
        out = dot(high, z_table[0], NN) + dot(high, z_table[1], NN) + dot(low, z_table[0], NN)
        re, im = out[:, 0:GRID], out[:, GRID:]
        power = jnp.transpose((re * re + im * im).reshape(64, 8, GRID), (1, 0, 2))
        kx = pl.ds(pl.multiple_of(8 * chunk, 8), 8)
        mode = 0.5 * influence[kx] * power
        energy[kx] = mode
        pltpu.make_async_copy(energy.at[kx], energy_hbm.at[kx], store_sem.at[chunk]).start()
        return total + jnp.sum(mode.reshape(64, 8, GRID), axis=0)

    total = lax.fori_loop(0, CHUNKS, modes_of, jnp.zeros((8, GRID), F32))

    evec[...] = total
    e_copies = []
    for off in range(1, 8):
        peer = lax.rem(me + off, 8)
        copy = pltpu.make_async_remote_copy(
            src_ref=evec, dst_ref=erecv.at[me], send_sem=e_send.at[off], recv_sem=e_recv.at[off],
            device_id=(0, peer // 4, lax.rem(peer, 4)), device_id_type=MESH)
        copy.start()
        e_copies.append(copy)
    erecv[me] = total
    for copy in e_copies:
        copy.wait_recv()
    grand = erecv[0]
    for n in range(1, 8):
        grand = grand + erecv[n]
    total_out[0] = jnp.sum(grand) * (1.0 / (GRID * GRID * GRID))

    for copy in ghosts + [copy for copies in a_copies for copy in copies] + e_copies:
        copy.wait_send()
    for chunk in range(CHUNKS):
        kx = pl.ds(8 * chunk, 8)
        pltpu.make_async_copy(energy.at[kx], energy_hbm.at[kx], store_sem.at[chunk]).wait()


def solution(mesh):
    slot_spec = P(('sys', 'ydom', 'zdom'))
    mode_spec = P(('sys', 'ydom'), 'zdom', None)
    x_table, z_table = dft_tables()

    def local_energy(charge, real_mask, grid_idx, spline_w, influence):
        slots = charge.shape[0]
        blocks = slots // BLOCK
        vmem = pl.BlockSpec(memory_space=pltpu.VMEM)
        hbm = pl.BlockSpec(memory_space=pl.ANY)
        groups = len(PAIRS)
        return pl.pallas_call(
            functools.partial(kernel, blocks),
            name='pme',
            out_shape=(jax.ShapeDtypeStruct(influence.shape, F32), jax.ShapeDtypeStruct((1,), F32)),
            in_specs=[vmem] * 4 + [hbm] * 3,
            out_specs=(hbm, pl.BlockSpec(memory_space=pltpu.SMEM)),
            scratch_shapes=[
                pltpu.VMEM(influence.shape, F32),
                pltpu.VMEM(x_table.shape, BF16),
                pltpu.VMEM(z_table.shape, BF16),
                pltpu.VMEM(influence.shape, F32),
                pltpu.VMEM((blocks, 2 * GRID, BLOCK), BF16),
                pltpu.VMEM((blocks, Y_ROWS, BLOCK), F32),
                pltpu.VMEM((blocks, LEN_Z, BLOCK), F32),
                pltpu.VMEM((max(map(len, PAIRS)) * 2 * LEN_Z, GRID), F32),
                pltpu.VMEM((GHOST, LEN_Z, GRID), F32),
                pltpu.VMEM((GHOST, Y_ROWS, GRID), F32),
                pltpu.VMEM((GHOST, LEN_Z, GRID), F32),
                pltpu.VMEM((8 * LEN_Y, GRID), F32),
                pltpu.VMEM((8 * 8, GRID), F32),
                pltpu.VMEM((max(map(len, PAIRS)), 2 * GRID, GRID), F32),
                pltpu.VMEM((4, TILES, 8, GRID), jnp.int32),
                pltpu.VMEM((8, TILES, 8, GRID), jnp.int32),
                pltpu.VMEM((8, groups, 8, GRID), F32),
                pltpu.VMEM((2 * CHUNKS, 8, 8, 2, 8, GRID), F32),
                pltpu.VMEM((2, 64, 8, GRID), F32),
                pltpu.VMEM((8, GRID), F32),
                pltpu.VMEM((8, 8, GRID), F32),
                pltpu.SemaphoreType.DMA((3,)),
                pltpu.SemaphoreType.DMA((CHUNKS,)),
                pltpu.SemaphoreType.DMA((7,)),
                pltpu.SemaphoreType.DMA((7,)),
                pltpu.SemaphoreType.DMA((groups, 8)),
                pltpu.SemaphoreType.DMA((groups, 8)),
                pltpu.SemaphoreType.DMA((8,)),
                pltpu.SemaphoreType.DMA((8,)),
            ],
            compiler_params=pltpu.CompilerParams(collective_id=0, has_side_effects=True, vmem_limit_bytes=VMEM_LIMIT),
        )(charge.reshape(1, slots), real_mask.reshape(1, slots), grid_idx.T,
          jnp.transpose(spline_w, (1, 2, 0)), influence, jnp.asarray(x_table), jnp.asarray(z_table))

    return jax.shard_map(local_energy, mesh=mesh, in_specs=(slot_spec, slot_spec, P(('sys', 'ydom', 'zdom'), None), P(('sys', 'ydom', 'zdom'), None, None), mode_spec), out_specs=(mode_spec, P('sys')), check_vma=False)
```

```python
import functools
import math
import numpy as np
import jax
import jax.numpy as jnp
from jax import lax
from jax.experimental import pallas as pl
from jax.experimental.pallas import tpu as pltpu
from jax.sharding import PartitionSpec as P

MESH = pl.DeviceIdType.MESH
F32 = jnp.float32
BF16 = jnp.bfloat16
GRID = 128
LEN_Y = 32
LEN_Z = 64
GHOST = 3
BLOCK = 256
Y_ROWS = 40
CHUNKS = 4
UNROLL = 4
VMEM_LIMIT = 60 * 1024 * 1024
GROUP_B = ((2,), (3, 4), (5, 6), (0, 1), (7,))
PAIRS = tuple(tuple(bs) + tuple(8 + b for b in bs) for bs in GROUP_B)
OFFSET = tuple(sum(4 * len(p) + 1 for p in PAIRS[:g]) for g in range(len(PAIRS)))
TILES = sum(4 * len(p) + 1 for p in PAIRS)
PLACE = {pair: (g, OFFSET[g] + 4 * n) for g, pairs in enumerate(PAIRS) for n, pair in enumerate(pairs)}
NT = (((1,), (1,)), ((), ()))
NN = (((1,), (0,)), ((), ()))


def split_table(table):
    table = np.asarray(table, np.float32)
    high = table.astype(jnp.bfloat16)
    low = (table - high.astype(np.float32)).astype(jnp.bfloat16)
    return np.stack([high, low])


def dft_tables():
    k = np.arange(GRID)
    phase = 2.0 * np.pi * ((k[:, None] * k[None, :]) % GRID) / GRID
    cos, sin = np.cos(phase), np.sin(phase)
    x_table = np.concatenate([cos, -sin], axis=0)
    z_table = []
    for half in range(2):
        c = cos[64 * half:64 * half + 64]
        s = sin[64 * half:64 * half + 64]
        z_table.append(np.block([[c, -s], [s, c]]))
    return split_table(x_table), split_table(np.concatenate(z_table, axis=0))


def split(value):
    high = value.astype(BF16)
    low = (value - high.astype(F32)).astype(BF16)
    return high, low


def dot(a, b, dims):
    return lax.dot_general(a, b, dims, preferred_element_type=F32)


def taps(base, weights, rows):
    delta = lax.broadcasted_iota(jnp.int32, (rows, base.shape[1]), 0) - base
    out = jnp.where(delta == 3, weights[3:4], 0.0)
    for s in (2, 1, 0):
        out = jnp.where(delta == s, weights[s:s + 1], out)
    return out


def c_add(a, b):
    return a[0] + b[0], a[1] + b[1]


def c_sub(a, b):
    return a[0] - b[0], a[1] - b[1]


def c_mul(a, turn):
    turn = turn % 1.0
    if turn == 0.0:
        return a
    if turn == 0.25:
        return a[1], -a[0]
    if turn == 0.5:
        return -a[0], -a[1]
    if turn == 0.75:
        return -a[1], a[0]
    c, s = math.cos(2 * math.pi * turn), math.sin(2 * math.pi * turn)
    if turn == 0.125:
        return c * (a[0] + a[1]), c * (a[1] - a[0])
    return c * a[0] + s * a[1], c * a[1] - s * a[0]


def fft(values):
    n = len(values)
    if n == 1:
        return values
    even, odd = fft(values[0::2]), fft(values[1::2])
    turned = [c_mul(o, k / n) for k, o in enumerate(odd)]
    return [c_add(e, t) for e, t in zip(even, turned)] + [c_sub(e, t) for e, t in zip(even, turned)]


def kernel(blocks, charge_hbm, mask_hbm, index_hbm, spline_hbm, influence_hbm, x_table_hbm, z_table_hbm,
           energy_hbm, total_out,
           charge, mask, index, spline, influence, x_table, z_table, energy,
           xcat, yline, zline, acc, yghost, zghost, yface, zface, corner,
           modes, fsend, grecv, scale, mid, hbuf, evec, erecv,
           load_sem, store_sem, ghost_send, ghost_recv, a_send, a_recv, e_send, e_recv):
    i = lax.axis_index('ydom')
    j = lax.axis_index('zdom')
    me = j * 4 + i
    i_next = lax.rem(i + 1, 4)
    j_next = 1 - j

    barrier = pltpu.get_barrier_semaphore()
    for off in range(1, 8):
        peer = lax.rem(me + off, 8)
        pl.semaphore_signal(barrier, inc=1, device_id=(0, peer // 4, lax.rem(peer, 4)), device_id_type=MESH)

    loads = [pltpu.make_async_copy(src, dst, load_sem.at[n]) for n, (src, dst) in enumerate(
        [(spline_hbm, spline), (index_hbm, index), (charge_hbm, charge), (mask_hbm, mask),
         (x_table_hbm, x_table), (z_table_hbm, z_table), (influence_hbm, influence)])]
    for copy in loads:
        copy.start()

    yghost[...] = jnp.zeros_like(yghost)
    zghost[...] = jnp.zeros_like(zghost)
    zface[GHOST * LEN_Y:] = jnp.zeros((5 * LEN_Y, GRID), F32)
    corner[GHOST * 8:] = jnp.zeros((5 * 8, GRID), F32)
    for copy in loads[:4]:
        copy.wait()

    def prepare(step, carry):
        total = None
        for n in range(2):
            b = 2 * step + n
            lanes = pl.ds(pl.multiple_of(b * BLOCK, BLOCK), BLOCK)
            weight = charge[:, lanes] * mask[:, lanes].astype(F32)
            wx = spline[0, :, lanes] * weight
            delta = (lax.broadcasted_iota(jnp.int32, (GRID, BLOCK), 0) - index[0:1, lanes]) & (GRID - 1)
            line = jnp.where(delta == 3, wx[3:4], 0.0)
            for s in (2, 1, 0):
                line = jnp.where(delta == s, wx[s:s + 1], line)
            xhigh, xlow = split(line)
            xcat[b, 0:GRID] = xhigh
            xcat[b, GRID:2 * GRID] = xlow
            yl = taps(index[1:2, lanes], spline[1, :, lanes], Y_ROWS)
            yline[b] = yl
            zl = taps(index[2:3, lanes], spline[2, :, lanes], LEN_Z + 8)
            zline[b] = zl[0:LEN_Z]
            rows = [yl[LEN_Y + t:LEN_Y + t + 1] * zl[0:LEN_Z] for t in range(GHOST)]
            rows += [zl[LEN_Z + u:LEN_Z + u + 1] * yl for u in range(GHOST)]
            rows += [jnp.zeros((8, BLOCK), F32)]
            high, low = split(jnp.concatenate(rows, axis=0))
            both = dot(high, jnp.concatenate([xhigh, xlow], axis=0), NT)
            part = both[:, 0:GRID] + both[:, GRID:] + dot(low, xhigh, NT)
            total = part if total is None else total + part
        yghost[...] += total[0:GHOST * LEN_Z].reshape(GHOST, LEN_Z, GRID)
        zghost[...] += total[GHOST * LEN_Z:GHOST * LEN_Z + GHOST * Y_ROWS].reshape(GHOST, Y_ROWS, GRID)
        return carry

    lax.fori_loop(0, blocks // 2, prepare, 0)

    pl.semaphore_wait(barrier, 7)
    ghosts = []
    for n, (src, dst, peer) in enumerate(
            [(yghost, yface, (0, j, i_next))]
            + [(zghost.at[u, 0:LEN_Y], zface.at[LEN_Y * u:LEN_Y * u + LEN_Y], (0, j_next, i)) for u in range(GHOST)]
            + [(zghost.at[u, LEN_Y:Y_ROWS], corner.at[8 * u:8 * u + 8], (0, j_next, i_next)) for u in range(GHOST)]):
        copy = pltpu.make_async_remote_copy(
            src_ref=src, dst_ref=dst, send_sem=ghost_send.at[n], recv_sem=ghost_recv.at[n],
            device_id=peer, device_id_type=MESH)
        copy.start()
        ghosts.append(copy)

    def spread_rows(pairs):
        count = 2 * LEN_Z * len(pairs)
        acc[0:count] = jnp.zeros((count, GRID), F32)

        def body(step, carry):
            both, single = None, None
            for n in range(UNROLL):
                b = UNROLL * step + n
                zl = zline[b]
                high, low = split(jnp.concatenate(
                    [yline[b, 2 * pair + h:2 * pair + h + 1] * zl for pair in pairs for h in range(2)], axis=0))
                one, two = dot(high, xcat[b], NT), dot(low, xcat[b, 0:GRID], NT)
                both, single = (one, two) if both is None else (both + one, single + two)
            acc[0:count] += both[:, 0:GRID] + both[:, GRID:] + single
            return carry
        lax.fori_loop(0, blocks // UNROLL, body, 0)

    a_copies = []
    for group, pairs in enumerate(PAIRS):
        spread_rows(pairs)
        if group == 0:
            for copy in ghosts:
                copy.wait_recv()
            loads[4].wait()
        for n, pair in enumerate(pairs):
            for h in range(2):
                y, row = 2 * pair + h, 64 * (2 * n + h)
                if y < GHOST:
                    acc[row:row + LEN_Z] += yface[y]
                    acc[row:row + 8] += corner[pl.ds(y, 8, stride=8)]
                acc[row:row + 8] += zface[pl.ds(y, 8, stride=LEN_Y)]
        for n in range(len(pairs)):
            high, low = split(acc[128 * n:128 * n + 128])
            modes[n] = dot(x_table[0], high, NT) + dot(x_table[1], high, NT) + dot(x_table[0], low, NT)
        first, last = OFFSET[group], OFFSET[group] + 4 * len(pairs)
        for peer in range(4):
            at = [(n, c, 32 * peer + 8 * c) for n in range(len(pairs)) for c in range(CHUNKS)]
            top = jnp.full((8, GRID), 1e-30, F32)
            for n, c, row in at:
                top = jnp.maximum(top, jnp.maximum(jnp.abs(modes[n, row:row + 8]), jnp.abs(modes[n, GRID + row:GRID + row + 8])))
            code = jnp.ceil(jnp.log(top) * 1024.0)
            inverse = 32760.0 / jnp.exp(code * (1.0 / 1024.0))
            for n, c, row in at:
                re = jnp.round(modes[n, row:row + 8] * inverse).astype(jnp.int32)
                im = jnp.round(modes[n, GRID + row:GRID + row + 8] * inverse).astype(jnp.int32)
                fsend[peer, first + 4 * n + c] = (im << 16) | (re & 0xffff)
            fsend[peer, last] = code.astype(jnp.int32)
        copies = []
        for d, dj in ((2, 1), (2, 0), (1, 1), (3, 1), (1, 0), (3, 0), (0, 1)):
            peer, peer_j = lax.rem(i + d, 4), (j_next if dj else j)
            copy = pltpu.make_async_remote_copy(
                src_ref=fsend.at[peer, first:last + 1], dst_ref=grecv.at[me, first:last + 1],
                send_sem=a_send.at[group, 2 * d + dj], recv_sem=a_recv.at[group, 2 * d + dj],
                device_id=(0, peer_j, peer), device_id_type=MESH)
            copy.start()
            copies.append(copy)
        a_copies.append(copies)
        grecv[me, first:last + 1] = fsend[i, first:last + 1]

    for group, bs in enumerate(GROUP_B):
        for copy in a_copies[group]:
            copy.wait_recv()
        last = OFFSET[group] + 4 * len(PAIRS[group])
        for src in range(8):
            scale[src, group] = jnp.exp(grecv[src, last].astype(F32) * (1.0 / 1024.0)) * (1.0 / 32760.0)

        def first_stage(part, carry):
            half, chunk = part // CHUNKS, lax.rem(part, CHUNKS)
            for b in bs:
                values = []
                for a in range(8):
                    src = 4 * half + a // 2
                    word = grecv[src, PLACE[8 * (a % 2) + b][1] + chunk]
                    unit = scale[src, group]
                    values.append((((word << 16) >> 16).astype(F32) * unit, (word >> 16).astype(F32) * unit))
                for c, value in enumerate(fft(values)):
                    value = c_mul(value, b * c / 64)
                    mid[part, c, b, 0] = value[0]
                    mid[part, c, b, 1] = value[1]
            return carry
        lax.fori_loop(0, 2 * CHUNKS, first_stage, 0)

    low_half = lax.broadcasted_iota(jnp.int32, (8, GRID), 1) < 64
    sign = (1 - 2 * j).astype(F32)
    loads[5].wait()
    loads[6].wait()

    def modes_of(chunk, total):
        for half in range(2):
            for c in range(8):
                values = fft([(mid[CHUNKS * half + chunk, c, b, 0], mid[CHUNKS * half + chunk, c, b, 1]) for b in range(8)])
                for d, value in enumerate(values):
                    k = c + 8 * d
                    turned = c_mul(value, k / 128)
                    left = jnp.where(low_half, value[0], pltpu.roll(value[1], 64, 1))
                    right = jnp.where(low_half, pltpu.roll(turned[0], 64, 1), turned[1])
                    hbuf[half, k] = left + sign * right
        rows = jnp.concatenate([hbuf[0].reshape(512, GRID), hbuf[1].reshape(512, GRID)], axis=1)
        high, low = split(rows)
        out = dot(high, z_table[0], NN) + dot(high, z_table[1], NN) + dot(low, z_table[0], NN)
        re, im = out[:, 0:GRID], out[:, GRID:]
        power = jnp.transpose((re * re + im * im).reshape(64, 8, GRID), (1, 0, 2))
        kx = pl.ds(pl.multiple_of(8 * chunk, 8), 8)
        mode = 0.5 * influence[kx] * power
        energy[kx] = mode
        pltpu.make_async_copy(energy.at[kx], energy_hbm.at[kx], store_sem.at[chunk]).start()
        return total + jnp.sum(mode.reshape(64, 8, GRID), axis=0)

    total = lax.fori_loop(0, CHUNKS, modes_of, jnp.zeros((8, GRID), F32))

    evec[...] = total
    e_copies = []
    for off in range(1, 8):
        peer = lax.rem(me + off, 8)
        copy = pltpu.make_async_remote_copy(
            src_ref=evec, dst_ref=erecv.at[me], send_sem=e_send.at[off], recv_sem=e_recv.at[off],
            device_id=(0, peer // 4, lax.rem(peer, 4)), device_id_type=MESH)
        copy.start()
        e_copies.append(copy)
    erecv[me] = total
    for copy in e_copies:
        copy.wait_recv()
    grand = erecv[0]
    for n in range(1, 8):
        grand = grand + erecv[n]
    total_out[0] = jnp.sum(grand) * (1.0 / (GRID * GRID * GRID))

    for copy in ghosts + [copy for copies in a_copies for copy in copies] + e_copies:
        copy.wait_send()
    for chunk in range(CHUNKS):
        kx = pl.ds(8 * chunk, 8)
        pltpu.make_async_copy(energy.at[kx], energy_hbm.at[kx], store_sem.at[chunk]).wait()


def solution(mesh):
    slot_spec = P(('sys', 'ydom', 'zdom'))
    mode_spec = P(('sys', 'ydom'), 'zdom', None)
    x_table, z_table = dft_tables()

    def local_energy(charge, real_mask, grid_idx, spline_w, influence):
        slots = charge.shape[0]
        blocks = slots // BLOCK
        hbm = pl.BlockSpec(memory_space=pltpu.HBM)
        groups = len(PAIRS)
        return pl.pallas_call(
            functools.partial(kernel, blocks),
            name='pme',
            out_shape=(jax.ShapeDtypeStruct(influence.shape, F32), jax.ShapeDtypeStruct((1,), F32)),
            in_specs=[hbm] * 7,
            out_specs=(pl.BlockSpec(memory_space=pl.ANY), pl.BlockSpec(memory_space=pltpu.SMEM)),
            scratch_shapes=[
                pltpu.VMEM((1, slots), F32),
                pltpu.VMEM((1, slots), jnp.int32),
                pltpu.VMEM((3, slots), jnp.int32),
                pltpu.VMEM((3, 4, slots), F32),
                pltpu.VMEM(influence.shape, F32),
                pltpu.VMEM(x_table.shape, BF16),
                pltpu.VMEM(z_table.shape, BF16),
                pltpu.VMEM(influence.shape, F32),
                pltpu.VMEM((blocks, 2 * GRID, BLOCK), BF16),
                pltpu.VMEM((blocks, Y_ROWS, BLOCK), F32),
                pltpu.VMEM((blocks, LEN_Z, BLOCK), F32),
                pltpu.VMEM((max(map(len, PAIRS)) * 2 * LEN_Z, GRID), F32),
                pltpu.VMEM((GHOST, LEN_Z, GRID), F32),
                pltpu.VMEM((GHOST, Y_ROWS, GRID), F32),
                pltpu.VMEM((GHOST, LEN_Z, GRID), F32),
                pltpu.VMEM((8 * LEN_Y, GRID), F32),
                pltpu.VMEM((8 * 8, GRID), F32),
                pltpu.VMEM((max(map(len, PAIRS)), 2 * GRID, GRID), F32),
                pltpu.VMEM((4, TILES, 8, GRID), jnp.int32),
                pltpu.VMEM((8, TILES, 8, GRID), jnp.int32),
                pltpu.VMEM((8, groups, 8, GRID), F32),
                pltpu.VMEM((2 * CHUNKS, 8, 8, 2, 8, GRID), F32),
                pltpu.VMEM((2, 64, 8, GRID), F32),
                pltpu.VMEM((8, GRID), F32),
                pltpu.VMEM((8, 8, GRID), F32),
                pltpu.SemaphoreType.DMA((7,)),
                pltpu.SemaphoreType.DMA((CHUNKS,)),
                pltpu.SemaphoreType.DMA((7,)),
                pltpu.SemaphoreType.DMA((7,)),
                pltpu.SemaphoreType.DMA((groups, 8)),
                pltpu.SemaphoreType.DMA((groups, 8)),
                pltpu.SemaphoreType.DMA((8,)),
                pltpu.SemaphoreType.DMA((8,)),
            ],
            compiler_params=pltpu.CompilerParams(collective_id=0, has_side_effects=True, vmem_limit_bytes=VMEM_LIMIT),
        )(charge.reshape(1, slots), real_mask.reshape(1, slots), grid_idx.T,
          jnp.transpose(spline_w, (1, 2, 0)), influence, jnp.asarray(x_table), jnp.asarray(z_table))

    return jax.shard_map(local_energy, mesh=mesh, in_specs=(slot_spec, slot_spec, P(('sys', 'ydom', 'zdom'), None), P(('sys', 'ydom', 'zdom'), None, None), mode_spec), out_specs=(mode_spec, P('sys')), check_vma=False)
```

```python
import functools
import math
import numpy as np
import jax
import jax.numpy as jnp
from jax import lax
from jax.experimental import pallas as pl
from jax.experimental.pallas import tpu as pltpu
from jax.sharding import PartitionSpec as P

MESH = pl.DeviceIdType.MESH
F32 = jnp.float32
BF16 = jnp.bfloat16
GRID = 128
LEN_Y = 32
LEN_Z = 64
GHOST = 3
BLOCK = 256
Y_ROWS = 40
CHUNKS = 4
UNROLL = 4
VMEM_LIMIT = 28 * 1024 * 1024
GROUP_B = ((2,), (3, 4), (5, 6), (0, 1), (7,))
PAIRS = tuple(tuple(bs) + tuple(8 + b for b in bs) for bs in GROUP_B)
OFFSET = tuple(sum(4 * len(p) + 1 for p in PAIRS[:g]) for g in range(len(PAIRS)))
TILES = sum(4 * len(p) + 1 for p in PAIRS)
PLACE = {pair: (g, OFFSET[g] + 4 * n) for g, pairs in enumerate(PAIRS) for n, pair in enumerate(pairs)}
NT = (((1,), (1,)), ((), ()))
NN = (((1,), (0,)), ((), ()))


def split_table(table):
    table = np.asarray(table, np.float32)
    high = table.astype(jnp.bfloat16)
    low = (table - high.astype(np.float32)).astype(jnp.bfloat16)
    return np.stack([high, low])


def dft_tables():
    k = np.arange(GRID)
    phase = 2.0 * np.pi * ((k[:, None] * k[None, :]) % GRID) / GRID
    cos, sin = np.cos(phase), np.sin(phase)
    x_table = np.concatenate([cos, -sin], axis=0)
    z_table = []
    for half in range(2):
        c = cos[64 * half:64 * half + 64]
        s = sin[64 * half:64 * half + 64]
        z_table.append(np.block([[c, -s], [s, c]]))
    return split_table(x_table), split_table(np.concatenate(z_table, axis=0))


def split(value):
    high = value.astype(BF16)
    low = (value - high.astype(F32)).astype(BF16)
    return high, low


def dot(a, b, dims):
    return lax.dot_general(a, b, dims, preferred_element_type=F32)


def taps(base, weights, rows):
    delta = lax.broadcasted_iota(jnp.int32, (rows, base.shape[1]), 0) - base
    out = jnp.where(delta == 3, weights[3:4], 0.0)
    for s in (2, 1, 0):
        out = jnp.where(delta == s, weights[s:s + 1], out)
    return out


def c_add(a, b):
    return a[0] + b[0], a[1] + b[1]


def c_sub(a, b):
    return a[0] - b[0], a[1] - b[1]


def c_mul(a, turn):
    turn = turn % 1.0
    if turn == 0.0:
        return a
    if turn == 0.25:
        return a[1], -a[0]
    if turn == 0.5:
        return -a[0], -a[1]
    if turn == 0.75:
        return -a[1], a[0]
    c, s = math.cos(2 * math.pi * turn), math.sin(2 * math.pi * turn)
    if turn == 0.125:
        return c * (a[0] + a[1]), c * (a[1] - a[0])
    return c * a[0] + s * a[1], c * a[1] - s * a[0]


def fft(values):
    n = len(values)
    if n == 1:
        return values
    even, odd = fft(values[0::2]), fft(values[1::2])
    turned = [c_mul(o, k / n) for k, o in enumerate(odd)]
    return [c_add(e, t) for e, t in zip(even, turned)] + [c_sub(e, t) for e, t in zip(even, turned)]


def kernel(blocks, charge_hbm, mask_hbm, index_hbm, spline_hbm, influence_hbm, x_table_hbm, z_table_hbm,
           energy, total_out,
           charge, mask, index, spline, influence, x_table, z_table,
           xcat, yline, zline, acc, yghost, zghost, yface, zface, corner,
           modes, fsend, grecv, scale, mid, hbuf, evec, erecv,
           load_sem, ghost_send, ghost_recv, a_send, a_recv, e_send, e_recv):
    i = lax.axis_index('ydom')
    j = lax.axis_index('zdom')
    me = j * 4 + i
    i_next = lax.rem(i + 1, 4)
    j_next = 1 - j
    mate = i + 1 - 2 * lax.rem(i, 2)
    cross, cross_mate = lax.rem(i + 2, 4), lax.rem(mate + 2, 4)

    barrier = pltpu.get_barrier_semaphore()
    for off in range(1, 8):
        peer = lax.rem(me + off, 8)
        pl.semaphore_signal(barrier, inc=1, device_id=(0, peer // 4, lax.rem(peer, 4)), device_id_type=MESH)

    loads = [pltpu.make_async_copy(src, dst, load_sem.at[n]) for n, (src, dst) in enumerate(
        [(spline_hbm, spline), (index_hbm, index), (charge_hbm, charge), (mask_hbm, mask),
         (x_table_hbm, x_table), (z_table_hbm, z_table), (influence_hbm, influence)])]
    for copy in loads:
        copy.start()

    yghost[...] = jnp.zeros_like(yghost)
    zghost[...] = jnp.zeros_like(zghost)
    zface[GHOST * LEN_Y:] = jnp.zeros((5 * LEN_Y, GRID), F32)
    corner[GHOST * 8:] = jnp.zeros((5 * 8, GRID), F32)
    for copy in loads[:4]:
        copy.wait()

    def prepare(step, carry):
        total = None
        for n in range(2):
            b = 2 * step + n
            lanes = pl.ds(pl.multiple_of(b * BLOCK, BLOCK), BLOCK)
            weight = charge[:, lanes] * mask[:, lanes].astype(F32)
            wx = spline[0, :, lanes] * weight
            delta = (lax.broadcasted_iota(jnp.int32, (GRID, BLOCK), 0) - index[0:1, lanes]) & (GRID - 1)
            line = jnp.where(delta == 3, wx[3:4], 0.0)
            for s in (2, 1, 0):
                line = jnp.where(delta == s, wx[s:s + 1], line)
            xhigh, xlow = split(line)
            xcat[b, 0:GRID] = xhigh
            xcat[b, GRID:2 * GRID] = xlow
            yl = taps(index[1:2, lanes], spline[1, :, lanes], Y_ROWS)
            yline[b] = yl
            zl = taps(index[2:3, lanes], spline[2, :, lanes], LEN_Z + 8)
            zline[b] = zl[0:LEN_Z]
            rows = [yl[LEN_Y + t:LEN_Y + t + 1] * zl[0:LEN_Z] for t in range(GHOST)]
            rows += [zl[LEN_Z + u:LEN_Z + u + 1] * yl for u in range(GHOST)]
            rows += [jnp.zeros((8, BLOCK), F32)]
            high, low = split(jnp.concatenate(rows, axis=0))
            both = dot(high, jnp.concatenate([xhigh, xlow], axis=0), NT)
            part = both[:, 0:GRID] + both[:, GRID:] + dot(low, xhigh, NT)
            total = part if total is None else total + part
        yghost[...] += total[0:GHOST * LEN_Z].reshape(GHOST, LEN_Z, GRID)
        zghost[...] += total[GHOST * LEN_Z:GHOST * LEN_Z + GHOST * Y_ROWS].reshape(GHOST, Y_ROWS, GRID)
        return carry

    lax.fori_loop(0, blocks // 2, prepare, 0)

    pl.semaphore_wait(barrier, 7)
    ghosts = []
    for n, (src, dst, peer) in enumerate(
            [(yghost, yface, (0, j, i_next))]
            + [(zghost.at[u, 0:LEN_Y], zface.at[LEN_Y * u:LEN_Y * u + LEN_Y], (0, j_next, i)) for u in range(GHOST)]
            + [(zghost.at[u, LEN_Y:Y_ROWS], corner.at[8 * u:8 * u + 8], (0, j_next, i_next)) for u in range(GHOST)]):
        copy = pltpu.make_async_remote_copy(
            src_ref=src, dst_ref=dst, send_sem=ghost_send.at[n], recv_sem=ghost_recv.at[n],
            device_id=peer, device_id_type=MESH)
        copy.start()
        ghosts.append(copy)

    def spread_rows(pairs):
        count = 2 * LEN_Z * len(pairs)
        acc[0:count] = jnp.zeros((count, GRID), F32)

        def body(step, carry):
            both, single = None, None
            for n in range(UNROLL):
                b = UNROLL * step + n
                zl = zline[b]
                high, low = split(jnp.concatenate(
                    [yline[b, 2 * pair + h:2 * pair + h + 1] * zl for pair in pairs for h in range(2)], axis=0))
                one, two = dot(high, xcat[b], NT), dot(low, xcat[b, 0:GRID], NT)
                both, single = (one, two) if both is None else (both + one, single + two)
            acc[0:count] += both[:, 0:GRID] + both[:, GRID:] + single
            return carry
        lax.fori_loop(0, blocks // UNROLL, body, 0)

    a_copies = []
    for group, pairs in enumerate(PAIRS):
        spread_rows(pairs)
        if group == 0:
            for copy in ghosts:
                copy.wait_recv()
            loads[4].wait()
        for n, pair in enumerate(pairs):
            for h in range(2):
                y, row = 2 * pair + h, 64 * (2 * n + h)
                if y < GHOST:
                    acc[row:row + LEN_Z] += yface[y]
                    acc[row:row + 8] += corner[pl.ds(y, 8, stride=8)]
                acc[row:row + 8] += zface[pl.ds(y, 8, stride=LEN_Y)]
        for n in range(len(pairs)):
            high, low = split(acc[128 * n:128 * n + 128])
            modes[n] = dot(x_table[0], high, NT) + dot(x_table[1], high, NT) + dot(x_table[0], low, NT)
        first, last = OFFSET[group], OFFSET[group] + 4 * len(pairs)
        for peer in range(4):
            at = [(n, c, 32 * peer + 8 * c) for n in range(len(pairs)) for c in range(CHUNKS)]
            top = jnp.full((8, GRID), 1e-30, F32)
            for n, c, row in at:
                top = jnp.maximum(top, jnp.maximum(jnp.abs(modes[n, row:row + 8]), jnp.abs(modes[n, GRID + row:GRID + row + 8])))
            code = jnp.ceil(jnp.log(top) * 1024.0)
            inverse = 32760.0 / jnp.exp(code * (1.0 / 1024.0))
            for n, c, row in at:
                re = jnp.round(modes[n, row:row + 8] * inverse).astype(jnp.int32)
                im = jnp.round(modes[n, GRID + row:GRID + row + 8] * inverse).astype(jnp.int32)
                fsend[peer, first + 4 * n + c] = (im << 16) | (re & 0xffff)
            fsend[peer, last] = code.astype(jnp.int32)
        copies = []
        for n, (peer, peer_j) in enumerate(((cross, j), (i, j_next), (cross_mate, j), (mate, j_next), (mate, j),
                                            (cross, j_next), (cross_mate, j_next))):
            copy = pltpu.make_async_remote_copy(
                src_ref=fsend.at[peer, first:last + 1], dst_ref=grecv.at[me, first:last + 1],
                send_sem=a_send.at[group, n], recv_sem=a_recv.at[group, n],
                device_id=(0, peer_j, peer), device_id_type=MESH)
            copy.start()
            copies.append(copy)
        a_copies.append(copies)
        grecv[me, first:last + 1] = fsend[i, first:last + 1]

    for group, bs in enumerate(GROUP_B):
        for copy in a_copies[group]:
            copy.wait_recv()
        last = OFFSET[group] + 4 * len(PAIRS[group])
        for src in range(8):
            scale[src, group] = jnp.exp(grecv[src, last].astype(F32) * (1.0 / 1024.0)) * (1.0 / 32760.0)

        def first_stage(part, carry):
            half, chunk = part // CHUNKS, lax.rem(part, CHUNKS)
            for b in bs:
                values = []
                for a in range(8):
                    src = 4 * half + a // 2
                    word = grecv[src, PLACE[8 * (a % 2) + b][1] + chunk]
                    unit = scale[src, group]
                    values.append((((word << 16) >> 16).astype(F32) * unit, (word >> 16).astype(F32) * unit))
                for c, value in enumerate(fft(values)):
                    value = c_mul(value, b * c / 64)
                    mid[part, c, b, 0] = value[0]
                    mid[part, c, b, 1] = value[1]
            return carry
        lax.fori_loop(0, 2 * CHUNKS, first_stage, 0)

    low_half = lax.broadcasted_iota(jnp.int32, (8, GRID), 1) < 64
    sign = (1 - 2 * j).astype(F32)
    loads[5].wait()
    loads[6].wait()

    def modes_of(chunk, total):
        for half in range(2):
            for c in range(8):
                values = fft([(mid[CHUNKS * half + chunk, c, b, 0], mid[CHUNKS * half + chunk, c, b, 1]) for b in range(8)])
                for d, value in enumerate(values):
                    k = c + 8 * d
                    turned = c_mul(value, k / 128)
                    left = jnp.where(low_half, value[0], pltpu.roll(value[1], 64, 1))
                    right = jnp.where(low_half, pltpu.roll(turned[0], 64, 1), turned[1])
                    hbuf[half, k] = left + sign * right
        rows = jnp.concatenate([hbuf[0].reshape(512, GRID), hbuf[1].reshape(512, GRID)], axis=1)
        high, low = split(rows)
        out = dot(high, z_table[0], NN) + dot(high, z_table[1], NN) + dot(low, z_table[0], NN)
        re, im = out[:, 0:GRID], out[:, GRID:]
        power = jnp.transpose((re * re + im * im).reshape(64, 8, GRID), (1, 0, 2))
        kx = pl.ds(pl.multiple_of(8 * chunk, 8), 8)
        mode = 0.5 * influence[kx] * power
        energy[kx] = mode
        return total + jnp.sum(mode.reshape(64, 8, GRID), axis=0)

    total = lax.fori_loop(0, CHUNKS, modes_of, jnp.zeros((8, GRID), F32))

    evec[...] = total
    e_copies = []
    for off in range(1, 8):
        peer = lax.rem(me + off, 8)
        copy = pltpu.make_async_remote_copy(
            src_ref=evec, dst_ref=erecv.at[me], send_sem=e_send.at[off], recv_sem=e_recv.at[off],
            device_id=(0, peer // 4, lax.rem(peer, 4)), device_id_type=MESH)
        copy.start()
        e_copies.append(copy)
    erecv[me] = total
    for copy in e_copies:
        copy.wait_recv()
    grand = erecv[0]
    for n in range(1, 8):
        grand = grand + erecv[n]
    total_out[0] = jnp.sum(grand) * (1.0 / (GRID * GRID * GRID))

    for copy in ghosts + [copy for copies in a_copies for copy in copies] + e_copies:
        copy.wait_send()


def solution(mesh):
    slot_spec = P(('sys', 'ydom', 'zdom'))
    mode_spec = P(('sys', 'ydom'), 'zdom', None)
    x_table, z_table = dft_tables()

    def local_energy(charge, real_mask, grid_idx, spline_w, influence):
        slots = charge.shape[0]
        blocks = slots // BLOCK
        hbm = pl.BlockSpec(memory_space=pltpu.HBM)
        groups = len(PAIRS)
        return pl.pallas_call(
            functools.partial(kernel, blocks),
            name='pme',
            out_shape=(jax.ShapeDtypeStruct(influence.shape, F32), jax.ShapeDtypeStruct((1,), F32)),
            in_specs=[hbm] * 7,
            out_specs=(pl.BlockSpec(memory_space=pltpu.VMEM), pl.BlockSpec(memory_space=pltpu.SMEM)),
            scratch_shapes=[
                pltpu.VMEM((1, slots), F32),
                pltpu.VMEM((1, slots), jnp.int32),
                pltpu.VMEM((3, slots), jnp.int32),
                pltpu.VMEM((3, 4, slots), F32),
                pltpu.VMEM(influence.shape, F32),
                pltpu.VMEM(x_table.shape, BF16),
                pltpu.VMEM(z_table.shape, BF16),
                pltpu.VMEM((blocks, 2 * GRID, BLOCK), BF16),
                pltpu.VMEM((blocks, Y_ROWS, BLOCK), F32),
                pltpu.VMEM((blocks, LEN_Z, BLOCK), F32),
                pltpu.VMEM((max(map(len, PAIRS)) * 2 * LEN_Z, GRID), F32),
                pltpu.VMEM((GHOST, LEN_Z, GRID), F32),
                pltpu.VMEM((GHOST, Y_ROWS, GRID), F32),
                pltpu.VMEM((GHOST, LEN_Z, GRID), F32),
                pltpu.VMEM((8 * LEN_Y, GRID), F32),
                pltpu.VMEM((8 * 8, GRID), F32),
                pltpu.VMEM((max(map(len, PAIRS)), 2 * GRID, GRID), F32),
                pltpu.VMEM((4, TILES, 8, GRID), jnp.int32),
                pltpu.VMEM((8, TILES, 8, GRID), jnp.int32),
                pltpu.VMEM((8, groups, 8, GRID), F32),
                pltpu.VMEM((2 * CHUNKS, 8, 8, 2, 8, GRID), F32),
                pltpu.VMEM((2, 64, 8, GRID), F32),
                pltpu.VMEM((8, GRID), F32),
                pltpu.VMEM((8, 8, GRID), F32),
                pltpu.SemaphoreType.DMA((7,)),
                pltpu.SemaphoreType.DMA((7,)),
                pltpu.SemaphoreType.DMA((7,)),
                pltpu.SemaphoreType.DMA((groups, 8)),
                pltpu.SemaphoreType.DMA((groups, 8)),
                pltpu.SemaphoreType.DMA((8,)),
                pltpu.SemaphoreType.DMA((8,)),
            ],
            compiler_params=pltpu.CompilerParams(collective_id=0, has_side_effects=True, vmem_limit_bytes=VMEM_LIMIT),
        )(*[pltpu.with_memory_space_constraint(value, pltpu.HBM) for value in (
            charge.reshape(1, slots), real_mask.reshape(1, slots), grid_idx.T,
            jnp.transpose(spline_w, (1, 2, 0)), influence, jnp.asarray(x_table), jnp.asarray(z_table))])

    return jax.shard_map(local_energy, mesh=mesh, in_specs=(slot_spec, slot_spec, P(('sys', 'ydom', 'zdom'), None), P(('sys', 'ydom', 'zdom'), None, None), mode_spec), out_specs=(mode_spec, P('sys')), check_vma=False)
```

```python
import functools
import math
import numpy as np
import jax
import jax.numpy as jnp
from jax import lax
from jax.experimental import pallas as pl
from jax.experimental.pallas import tpu as pltpu
from jax.sharding import PartitionSpec as P

MESH = pl.DeviceIdType.MESH
F32 = jnp.float32
BF16 = jnp.bfloat16
GRID = 128
LEN_Y = 32
LEN_Z = 64
GHOST = 3
BLOCK = 256
Y_ROWS = 40
CHUNKS = 4
UNROLL = 8
VMEM_LIMIT = 28 * 1024 * 1024
GROUP_B = ((2, 3), (4, 5), (0, 1), (6,), (7,))
PAIRS = tuple(tuple(bs) + tuple(8 + b for b in bs) for bs in GROUP_B)
OFFSET = tuple(sum(4 * len(p) + 1 for p in PAIRS[:g]) for g in range(len(PAIRS)))
TILES = sum(4 * len(p) + 1 for p in PAIRS)
PLACE = {pair: (OFFSET[g] + 1 + n, len(pairs)) for g, pairs in enumerate(PAIRS) for n, pair in enumerate(pairs)}
NT = (((1,), (1,)), ((), ()))
NN = (((1,), (0,)), ((), ()))


def split_table(table):
    table = np.asarray(table, np.float32)
    high = table.astype(jnp.bfloat16)
    low = (table - high.astype(np.float32)).astype(jnp.bfloat16)
    return np.stack([high, low])


def dft_tables():
    k = np.arange(GRID)
    phase = 2.0 * np.pi * ((k[:, None] * k[None, :]) % GRID) / GRID
    cos, sin = np.cos(phase), np.sin(phase)
    x_table = np.concatenate([cos, -sin], axis=0)
    z_table = []
    for half in range(2):
        c = cos[64 * half:64 * half + 64]
        s = sin[64 * half:64 * half + 64]
        z_table.append(np.block([[c, -s], [s, c]]))
    return split_table(x_table), split_table(np.concatenate(z_table, axis=0))


def split(value):
    high = value.astype(BF16)
    low = (value - high.astype(F32)).astype(BF16)
    return high, low


def dot(a, b, dims):
    return lax.dot_general(a, b, dims, preferred_element_type=F32)


def taps(base, weights, rows):
    delta = lax.broadcasted_iota(jnp.int32, (rows, base.shape[1]), 0) - base
    out = jnp.where(delta == 3, weights[3:4], 0.0)
    for s in (2, 1, 0):
        out = jnp.where(delta == s, weights[s:s + 1], out)
    return out


def c_add(a, b):
    return a[0] + b[0], a[1] + b[1]


def c_sub(a, b):
    return a[0] - b[0], a[1] - b[1]


def c_mul(a, turn):
    turn = turn % 1.0
    if turn == 0.0:
        return a
    if turn == 0.25:
        return a[1], -a[0]
    if turn == 0.5:
        return -a[0], -a[1]
    if turn == 0.75:
        return -a[1], a[0]
    c, s = math.cos(2 * math.pi * turn), math.sin(2 * math.pi * turn)
    if turn == 0.125:
        return c * (a[0] + a[1]), c * (a[1] - a[0])
    return c * a[0] + s * a[1], c * a[1] - s * a[0]


def fft(values):
    n = len(values)
    if n == 1:
        return values
    even, odd = fft(values[0::2]), fft(values[1::2])
    turned = [c_mul(o, k / n) for k, o in enumerate(odd)]
    return [c_add(e, t) for e, t in zip(even, turned)] + [c_sub(e, t) for e, t in zip(even, turned)]


def kernel(blocks, charge_hbm, mask_hbm, index_hbm, spline_hbm, influence_hbm, x_table_hbm, z_table_hbm,
           energy, total_out,
           charge, mask, index, spline, influence, x_table, z_table,
           xcat, yline, zline, acc, yghost, zghost, yface, zface, corner,
           modes, fsend, grecv, scale, mid, hbuf, evec, erecv,
           load_sem, ghost_send, ghost_recv, a_send, a_recv, e_send, e_recv):
    i = lax.axis_index('ydom')
    j = lax.axis_index('zdom')
    me = j * 4 + i
    i_next = lax.rem(i + 1, 4)
    j_next = 1 - j
    mate = i + 1 - 2 * lax.rem(i, 2)
    cross, cross_mate = lax.rem(i + 2, 4), lax.rem(mate + 2, 4)

    barrier = pltpu.get_barrier_semaphore()
    for off in range(1, 8):
        peer = lax.rem(me + off, 8)
        pl.semaphore_signal(barrier, inc=1, device_id=(0, peer // 4, lax.rem(peer, 4)), device_id_type=MESH)

    loads = [pltpu.make_async_copy(src, dst, load_sem.at[n]) for n, (src, dst) in enumerate(
        [(spline_hbm, spline), (index_hbm, index), (charge_hbm, charge), (mask_hbm, mask),
         (x_table_hbm, x_table), (z_table_hbm, z_table), (influence_hbm, influence)])]
    for copy in loads:
        copy.start()

    yghost[...] = jnp.zeros_like(yghost)
    zghost[...] = jnp.zeros_like(zghost)
    zface[GHOST * LEN_Y:] = jnp.zeros((5 * LEN_Y, GRID), F32)
    corner[GHOST * 8:] = jnp.zeros((5 * 8, GRID), F32)
    for copy in loads[:4]:
        copy.wait()

    def prepare(step, carry):
        total = None
        for n in range(2):
            b = 2 * step + n
            lanes = pl.ds(pl.multiple_of(b * BLOCK, BLOCK), BLOCK)
            weight = charge[:, lanes] * mask[:, lanes].astype(F32)
            wx = spline[0, :, lanes] * weight
            delta = (lax.broadcasted_iota(jnp.int32, (GRID, BLOCK), 0) - index[0:1, lanes]) & (GRID - 1)
            line = jnp.where(delta == 3, wx[3:4], 0.0)
            for s in (2, 1, 0):
                line = jnp.where(delta == s, wx[s:s + 1], line)
            xhigh, xlow = split(line)
            xcat[b, 0:GRID] = xhigh
            xcat[b, GRID:2 * GRID] = xlow
            yl = taps(index[1:2, lanes], spline[1, :, lanes], Y_ROWS)
            yline[b] = yl
            zl = taps(index[2:3, lanes], spline[2, :, lanes], LEN_Z + 8)
            zline[b] = zl[0:LEN_Z]
            rows = [yl[LEN_Y + t:LEN_Y + t + 1] * zl[0:LEN_Z] for t in range(GHOST)]
            rows += [zl[LEN_Z + u:LEN_Z + u + 1] * yl for u in range(GHOST)]
            rows += [jnp.zeros((8, BLOCK), F32)]
            high, low = split(jnp.concatenate(rows, axis=0))
            both = dot(high, jnp.concatenate([xhigh, xlow], axis=0), NT)
            part = both[:, 0:GRID] + both[:, GRID:] + dot(low, xhigh, NT)
            total = part if total is None else total + part
        yghost[...] += total[0:GHOST * LEN_Z].reshape(GHOST, LEN_Z, GRID)
        zghost[...] += total[GHOST * LEN_Z:GHOST * LEN_Z + GHOST * Y_ROWS].reshape(GHOST, Y_ROWS, GRID)
        return carry

    lax.fori_loop(0, blocks // 2, prepare, 0)

    pl.semaphore_wait(barrier, 7)
    ghosts = []
    for n, (src, dst, peer) in enumerate(
            [(yghost, yface, (0, j, i_next))]
            + [(zghost.at[u, 0:LEN_Y], zface.at[LEN_Y * u:LEN_Y * u + LEN_Y], (0, j_next, i)) for u in range(GHOST)]
            + [(zghost.at[u, LEN_Y:Y_ROWS], corner.at[8 * u:8 * u + 8], (0, j_next, i_next)) for u in range(GHOST)]):
        copy = pltpu.make_async_remote_copy(
            src_ref=src, dst_ref=dst, send_sem=ghost_send.at[n], recv_sem=ghost_recv.at[n],
            device_id=peer, device_id_type=MESH)
        copy.start()
        ghosts.append(copy)

    def spread_rows(pairs):
        count = 2 * LEN_Z * len(pairs)
        acc[0:count] = jnp.zeros((count, GRID), F32)

        def body(step, carry):
            both, single = None, None
            for n in range(UNROLL):
                b = UNROLL * step + n
                zl = zline[b]
                high, low = split(jnp.concatenate(
                    [yline[b, 2 * pair + h:2 * pair + h + 1] * zl for pair in pairs for h in range(2)], axis=0))
                one, two = dot(high, xcat[b], NT), dot(low, xcat[b, 0:GRID], NT)
                both, single = (one, two) if both is None else (both + one, single + two)
            acc[0:count] += both[:, 0:GRID] + both[:, GRID:] + single
            return carry
        lax.fori_loop(0, blocks // UNROLL, body, 0)

    a_copies = []
    for group, pairs in enumerate(PAIRS):
        spread_rows(pairs)
        if group == 0:
            for copy in ghosts:
                copy.wait_recv()
            loads[4].wait()
        for n, pair in enumerate(pairs):
            for h in range(2):
                y, row = 2 * pair + h, 64 * (2 * n + h)
                if y < GHOST:
                    acc[row:row + LEN_Z] += yface[y]
                    acc[row:row + 8] += corner[pl.ds(y, 8, stride=8)]
                acc[row:row + 8] += zface[pl.ds(y, 8, stride=LEN_Y)]
        for n in range(len(pairs)):
            high, low = split(acc[128 * n:128 * n + 128])
            modes[n] = dot(x_table[0], high, NT) + dot(x_table[1], high, NT) + dot(x_table[0], low, NT)
        first, count = OFFSET[group], len(pairs)
        for peer in range(4):
            at = [(n, c, 32 * peer + 8 * c) for n in range(len(pairs)) for c in range(CHUNKS)]
            top = jnp.full((8, GRID), 1e-30, F32)
            for n, c, row in at:
                top = jnp.maximum(top, jnp.maximum(jnp.abs(modes[n, row:row + 8]), jnp.abs(modes[n, GRID + row:GRID + row + 8])))
            code = jnp.ceil(jnp.log(top) * 1024.0)
            inverse = 32760.0 / jnp.exp(code * (1.0 / 1024.0))
            for n, c, row in at:
                re = jnp.round(modes[n, row:row + 8] * inverse).astype(jnp.int32)
                im = jnp.round(modes[n, GRID + row:GRID + row + 8] * inverse).astype(jnp.int32)
                fsend[peer, first + 1 + count * c + n] = (im << 16) | (re & 0xffff)
            fsend[peer, first] = code.astype(jnp.int32)
        if group < len(PAIRS) - 1:
            slabs = [(first, first + 1 + 4 * count)]
        else:
            slabs = [(first + 1 + count * c - (c == 0), first + 1 + count * (c + 1)) for c in range(CHUNKS)]
        for start, stop in slabs:
            copies = []
            for n, (peer, peer_j) in enumerate(((cross, j), (i, j_next), (cross_mate, j), (mate, j_next), (mate, j),
                                                (cross, j_next), (cross_mate, j_next))):
                copy = pltpu.make_async_remote_copy(
                    src_ref=fsend.at[peer, start:stop], dst_ref=grecv.at[me, start:stop],
                    send_sem=a_send.at[len(a_copies), n], recv_sem=a_recv.at[len(a_copies), n],
                    device_id=(0, peer_j, peer), device_id_type=MESH)
                copy.start()
                copies.append(copy)
            a_copies.append(copies)
        stop = first + 1 + 4 * count
        grecv[me, first:stop] = fsend[i, first:stop]

    def unit_of(group):
        for src in range(8):
            scale[src, group] = jnp.exp(grecv[src, OFFSET[group]].astype(F32) * (1.0 / 1024.0)) * (1.0 / 32760.0)

    def first_stage(group, half, chunk):
        part = CHUNKS * half + chunk
        for b in GROUP_B[group]:
            values = []
            for a in range(8):
                src = 4 * half + a // 2
                tile, count = PLACE[8 * (a % 2) + b]
                word = grecv[src, tile + count * chunk]
                unit = scale[src, group]
                values.append((((word << 16) >> 16).astype(F32) * unit, (word >> 16).astype(F32) * unit))
            for c, value in enumerate(fft(values)):
                value = c_mul(value, b * c / 64)
                mid[part, c, b, 0] = value[0]
                mid[part, c, b, 1] = value[1]

    last = len(GROUP_B) - 1
    for group in range(last):
        for copy in a_copies[group]:
            copy.wait_recv()
        unit_of(group)

        def stage_part(part, carry):
            first_stage(group, part // CHUNKS, lax.rem(part, CHUNKS))
            return carry
        lax.fori_loop(0, 2 * CHUNKS, stage_part, 0)

    low_half = lax.broadcasted_iota(jnp.int32, (8, GRID), 1) < 64
    sign = (1 - 2 * j).astype(F32)
    loads[5].wait()
    loads[6].wait()

    def modes_of(chunk, total):
        for half in range(2):
            for c in range(8):
                values = fft([(mid[CHUNKS * half + chunk, c, b, 0], mid[CHUNKS * half + chunk, c, b, 1]) for b in range(8)])
                for d, value in enumerate(values):
                    k = c + 8 * d
                    turned = c_mul(value, k / 128)
                    left = jnp.where(low_half, value[0], pltpu.roll(value[1], 64, 1))
                    right = jnp.where(low_half, pltpu.roll(turned[0], 64, 1), turned[1])
                    hbuf[half, k] = left + sign * right
        rows = jnp.concatenate([hbuf[0].reshape(512, GRID), hbuf[1].reshape(512, GRID)], axis=1)
        high, low = split(rows)
        out = dot(high, z_table[0], NN) + dot(high, z_table[1], NN) + dot(low, z_table[0], NN)
        re, im = out[:, 0:GRID], out[:, GRID:]
        power = jnp.transpose((re * re + im * im).reshape(64, 8, GRID), (1, 0, 2))
        kx = pl.ds(8 * chunk, 8)
        mode = 0.5 * influence[kx] * power
        energy[kx] = mode
        return total + jnp.sum(mode.reshape(64, 8, GRID), axis=0)

    total = jnp.zeros((8, GRID), F32)
    for chunk in range(CHUNKS):
        for copy in a_copies[last + chunk]:
            copy.wait_recv()
        if chunk == 0:
            unit_of(last)
        for half in range(2):
            first_stage(last, half, chunk)
        total = modes_of(chunk, total)

    evec[...] = total
    e_copies = []
    for off in range(1, 8):
        peer = lax.rem(me + off, 8)
        copy = pltpu.make_async_remote_copy(
            src_ref=evec, dst_ref=erecv.at[me], send_sem=e_send.at[off], recv_sem=e_recv.at[off],
            device_id=(0, peer // 4, lax.rem(peer, 4)), device_id_type=MESH)
        copy.start()
        e_copies.append(copy)
    erecv[me] = total
    for copy in e_copies:
        copy.wait_recv()
    grand = erecv[0]
    for n in range(1, 8):
        grand = grand + erecv[n]
    total_out[0] = jnp.sum(grand) * (1.0 / (GRID * GRID * GRID))

    for copy in ghosts + [copy for copies in a_copies for copy in copies] + e_copies:
        copy.wait_send()


def solution(mesh):
    slot_spec = P(('sys', 'ydom', 'zdom'))
    mode_spec = P(('sys', 'ydom'), 'zdom', None)
    x_table, z_table = dft_tables()

    def local_energy(charge, real_mask, grid_idx, spline_w, influence):
        slots = charge.shape[0]
        blocks = slots // BLOCK
        hbm = pl.BlockSpec(memory_space=pltpu.HBM)
        groups = len(PAIRS)
        return pl.pallas_call(
            functools.partial(kernel, blocks),
            name='pme',
            out_shape=(jax.ShapeDtypeStruct(influence.shape, F32), jax.ShapeDtypeStruct((1,), F32)),
            in_specs=[hbm] * 7,
            out_specs=(pl.BlockSpec(memory_space=pltpu.VMEM), pl.BlockSpec(memory_space=pltpu.SMEM)),
            scratch_shapes=[
                pltpu.VMEM((1, slots), F32),
                pltpu.VMEM((1, slots), jnp.int32),
                pltpu.VMEM((3, slots), jnp.int32),
                pltpu.VMEM((3, 4, slots), F32),
                pltpu.VMEM(influence.shape, F32),
                pltpu.VMEM(x_table.shape, BF16),
                pltpu.VMEM(z_table.shape, BF16),
                pltpu.VMEM((blocks, 2 * GRID, BLOCK), BF16),
                pltpu.VMEM((blocks, Y_ROWS, BLOCK), F32),
                pltpu.VMEM((blocks, LEN_Z, BLOCK), F32),
                pltpu.VMEM((max(map(len, PAIRS)) * 2 * LEN_Z, GRID), F32),
                pltpu.VMEM((GHOST, LEN_Z, GRID), F32),
                pltpu.VMEM((GHOST, Y_ROWS, GRID), F32),
                pltpu.VMEM((GHOST, LEN_Z, GRID), F32),
                pltpu.VMEM((8 * LEN_Y, GRID), F32),
                pltpu.VMEM((8 * 8, GRID), F32),
                pltpu.VMEM((max(map(len, PAIRS)), 2 * GRID, GRID), F32),
                pltpu.VMEM((4, TILES, 8, GRID), jnp.int32),
                pltpu.VMEM((8, TILES, 8, GRID), jnp.int32),
                pltpu.VMEM((8, groups, 8, GRID), F32),
                pltpu.VMEM((2 * CHUNKS, 8, 8, 2, 8, GRID), F32),
                pltpu.VMEM((2, 64, 8, GRID), F32),
                pltpu.VMEM((8, GRID), F32),
                pltpu.VMEM((8, 8, GRID), F32),
                pltpu.SemaphoreType.DMA((7,)),
                pltpu.SemaphoreType.DMA((7,)),
                pltpu.SemaphoreType.DMA((7,)),
                pltpu.SemaphoreType.DMA((groups + CHUNKS - 1, 7)),
                pltpu.SemaphoreType.DMA((groups + CHUNKS - 1, 7)),
                pltpu.SemaphoreType.DMA((8,)),
                pltpu.SemaphoreType.DMA((8,)),
            ],
            compiler_params=pltpu.CompilerParams(collective_id=0, has_side_effects=True, vmem_limit_bytes=VMEM_LIMIT),
        )(*[pltpu.with_memory_space_constraint(value, pltpu.HBM) for value in (
            charge.reshape(1, slots), real_mask.reshape(1, slots), grid_idx.T,
            jnp.transpose(spline_w, (1, 2, 0)), influence, jnp.asarray(x_table), jnp.asarray(z_table))])

    return jax.shard_map(local_energy, mesh=mesh, in_specs=(slot_spec, slot_spec, P(('sys', 'ydom', 'zdom'), None), P(('sys', 'ydom', 'zdom'), None, None), mode_spec), out_specs=(mode_spec, P('sys')), check_vma=False)
```

```python
import functools
import math
import numpy as np
import jax
import jax.numpy as jnp
from jax import lax
from jax.experimental import pallas as pl
from jax.experimental.pallas import tpu as pltpu
from jax.sharding import PartitionSpec as P

MESH = pl.DeviceIdType.MESH
F32 = jnp.float32
BF16 = jnp.bfloat16
GRID = 128
LEN_Y = 32
LEN_Z = 64
GHOST = 3
BLOCK = 256
Y_ROWS = 40
CHUNKS = 4
UNROLL = 8
VMEM_LIMIT = 28 * 1024 * 1024
GROUP_B = ((2, 3), (4, 5), (0, 1), (6,), (7,))
PAIRS = tuple(tuple(bs) + tuple(8 + b for b in bs) for bs in GROUP_B)
OFFSET = tuple(sum(4 * len(p) + 1 for p in PAIRS[:g]) for g in range(len(PAIRS)))
TILES = sum(4 * len(p) + 1 for p in PAIRS)
PLACE = {pair: (OFFSET[g] + 1 + n, len(pairs)) for g, pairs in enumerate(PAIRS) for n, pair in enumerate(pairs)}
NT = (((1,), (1,)), ((), ()))
NN = (((1,), (0,)), ((), ()))


def split_table(table):
    table = np.asarray(table, np.float32)
    high = table.astype(jnp.bfloat16)
    low = (table - high.astype(np.float32)).astype(jnp.bfloat16)
    return np.stack([high, low])


def dft_tables():
    k = np.arange(GRID)
    phase = 2.0 * np.pi * ((k[:, None] * k[None, :]) % GRID) / GRID
    cos, sin = np.cos(phase), np.sin(phase)
    x_table = np.concatenate([cos, -sin], axis=0)
    z_table = []
    for half in range(2):
        c = cos[64 * half:64 * half + 64]
        s = sin[64 * half:64 * half + 64]
        z_table.append(np.block([[c, -s], [s, c]]))
    return split_table(x_table), split_table(np.concatenate(z_table, axis=0))


def split(value):
    high = value.astype(BF16)
    low = (value - high.astype(F32)).astype(BF16)
    return high, low


def dot(a, b, dims):
    return lax.dot_general(a, b, dims, preferred_element_type=F32)


def taps(base, weights, rows):
    delta = lax.broadcasted_iota(jnp.int32, (rows, base.shape[1]), 0) - base
    out = jnp.where(delta == 3, weights[3:4], 0.0)
    for s in (2, 1, 0):
        out = jnp.where(delta == s, weights[s:s + 1], out)
    return out


def c_add(a, b):
    return a[0] + b[0], a[1] + b[1]


def c_sub(a, b):
    return a[0] - b[0], a[1] - b[1]


def c_mul(a, turn):
    turn = turn % 1.0
    if turn == 0.0:
        return a
    if turn == 0.25:
        return a[1], -a[0]
    if turn == 0.5:
        return -a[0], -a[1]
    if turn == 0.75:
        return -a[1], a[0]
    c, s = math.cos(2 * math.pi * turn), math.sin(2 * math.pi * turn)
    if turn == 0.125:
        return c * (a[0] + a[1]), c * (a[1] - a[0])
    return c * a[0] + s * a[1], c * a[1] - s * a[0]


def fft(values):
    n = len(values)
    if n == 1:
        return values
    even, odd = fft(values[0::2]), fft(values[1::2])
    turned = [c_mul(o, k / n) for k, o in enumerate(odd)]
    return [c_add(e, t) for e, t in zip(even, turned)] + [c_sub(e, t) for e, t in zip(even, turned)]


def kernel(blocks, charge_hbm, mask_hbm, index_hbm, spline_hbm, influence_hbm, x_table_hbm, z_table_hbm,
           energy, total_out,
           charge, mask, index, spline, influence, x_table, z_table,
           xcat, yline, zline, acc, yghost, zghost, yface, zface, corner,
           modes, fsend, grecv, scale, mid, hbuf, evec, erecv,
           load_sem, ghost_send, ghost_recv, a_send, a_recv, e_send, e_recv):
    i = lax.axis_index('ydom')
    j = lax.axis_index('zdom')
    me = j * 4 + i
    i_next = lax.rem(i + 1, 4)
    j_next = 1 - j
    mate = i + 1 - 2 * lax.rem(i, 2)
    cross, cross_mate = lax.rem(i + 2, 4), lax.rem(mate + 2, 4)

    barrier = pltpu.get_barrier_semaphore()
    for off in range(1, 8):
        peer = lax.rem(me + off, 8)
        pl.semaphore_signal(barrier, inc=1, device_id=(0, peer // 4, lax.rem(peer, 4)), device_id_type=MESH)

    loads = [pltpu.make_async_copy(src, dst, load_sem.at[n]) for n, (src, dst) in enumerate(
        [(spline_hbm, spline), (index_hbm, index), (charge_hbm, charge), (mask_hbm, mask),
         (x_table_hbm, x_table), (z_table_hbm, z_table), (influence_hbm, influence)])]
    for copy in loads:
        copy.start()

    yghost[...] = jnp.zeros_like(yghost)
    zghost[...] = jnp.zeros_like(zghost)
    zface[GHOST * LEN_Y:] = jnp.zeros((5 * LEN_Y, GRID), F32)
    corner[GHOST * 8:] = jnp.zeros((5 * 8, GRID), F32)
    for copy in loads[:4]:
        copy.wait()

    def prepare(step, carry):
        total = None
        for n in range(4):
            b = 4 * step + n
            lanes = pl.ds(pl.multiple_of(b * BLOCK, BLOCK), BLOCK)
            weight = charge[:, lanes] * mask[:, lanes].astype(F32)
            wx = spline[0, :, lanes] * weight
            delta = (lax.broadcasted_iota(jnp.int32, (GRID, BLOCK), 0) - index[0:1, lanes]) & (GRID - 1)
            line = jnp.where(delta == 3, wx[3:4], 0.0)
            for s in (2, 1, 0):
                line = jnp.where(delta == s, wx[s:s + 1], line)
            xhigh, xlow = split(line)
            xcat[b, 0:GRID] = xhigh
            xcat[b, GRID:2 * GRID] = xlow
            yl = taps(index[1:2, lanes], spline[1, :, lanes], Y_ROWS)
            yline[b] = yl
            zl = taps(index[2:3, lanes], spline[2, :, lanes], LEN_Z + 8)
            zline[b] = zl[0:LEN_Z]
            rows = [yl[LEN_Y + t:LEN_Y + t + 1] * zl[0:LEN_Z] for t in range(GHOST)]
            rows += [zl[LEN_Z + u:LEN_Z + u + 1] * yl for u in range(GHOST)]
            rows += [jnp.zeros((8, BLOCK), F32)]
            high, low = split(jnp.concatenate(rows, axis=0))
            cat = jnp.concatenate([xhigh, xlow], axis=0)
            part = dot(high, cat, NT) + dot(low, cat, NT)
            total = part if total is None else total + part
        total = total[:, 0:GRID] + total[:, GRID:]
        yghost[...] += total[0:GHOST * LEN_Z].reshape(GHOST, LEN_Z, GRID)
        zghost[...] += total[GHOST * LEN_Z:GHOST * LEN_Z + GHOST * Y_ROWS].reshape(GHOST, Y_ROWS, GRID)
        return carry

    lax.fori_loop(0, blocks // 4, prepare, 0)

    pl.semaphore_wait(barrier, 7)
    ghosts = []
    for n, (src, dst, peer) in enumerate(
            [(yghost, yface, (0, j, i_next))]
            + [(zghost.at[u, 0:LEN_Y], zface.at[LEN_Y * u:LEN_Y * u + LEN_Y], (0, j_next, i)) for u in range(GHOST)]
            + [(zghost.at[u, LEN_Y:Y_ROWS], corner.at[8 * u:8 * u + 8], (0, j_next, i_next)) for u in range(GHOST)]):
        copy = pltpu.make_async_remote_copy(
            src_ref=src, dst_ref=dst, send_sem=ghost_send.at[n], recv_sem=ghost_recv.at[n],
            device_id=peer, device_id_type=MESH)
        copy.start()
        ghosts.append(copy)

    def spread_rows(pairs):
        count = 2 * LEN_Z * len(pairs)
        acc[0:count] = jnp.zeros((count, GRID), F32)

        def body(step, carry):
            both = None
            for n in range(UNROLL):
                b = UNROLL * step + n
                zl = zline[b]
                high, low = split(jnp.concatenate(
                    [yline[b, 2 * pair + h:2 * pair + h + 1] * zl for pair in pairs for h in range(2)], axis=0))
                part = dot(high, xcat[b], NT) + dot(low, xcat[b], NT)
                both = part if both is None else both + part
            acc[0:count] += both[:, 0:GRID] + both[:, GRID:]
            return carry
        lax.fori_loop(0, blocks // UNROLL, body, 0)

    a_copies = []
    for group, pairs in enumerate(PAIRS):
        spread_rows(pairs)
        if group == 0:
            for copy in ghosts:
                copy.wait_recv()
            loads[4].wait()
        for n, pair in enumerate(pairs):
            for h in range(2):
                y, row = 2 * pair + h, 64 * (2 * n + h)
                if y < GHOST:
                    acc[row:row + LEN_Z] += yface[y]
                    acc[row:row + 8] += corner[pl.ds(y, 8, stride=8)]
                acc[row:row + 8] += zface[pl.ds(y, 8, stride=LEN_Y)]
        for n in range(len(pairs)):
            high, low = split(acc[128 * n:128 * n + 128])
            modes[n] = dot(x_table[0], high, NT) + dot(x_table[1], high, NT) + dot(x_table[0], low, NT)
        first, count = OFFSET[group], len(pairs)
        for peer in range(4):
            at = [(n, c, 32 * peer + 8 * c) for n in range(len(pairs)) for c in range(CHUNKS)]
            top = jnp.full((8, GRID), 1e-30, F32)
            for n, c, row in at:
                top = jnp.maximum(top, jnp.maximum(jnp.abs(modes[n, row:row + 8]), jnp.abs(modes[n, GRID + row:GRID + row + 8])))
            code = jnp.ceil(jnp.log(top) * 1024.0)
            inverse = 32760.0 / jnp.exp(code * (1.0 / 1024.0))
            for n, c, row in at:
                re = jnp.round(modes[n, row:row + 8] * inverse).astype(jnp.int32)
                im = jnp.round(modes[n, GRID + row:GRID + row + 8] * inverse).astype(jnp.int32)
                fsend[peer, first + 1 + count * c + n] = (im << 16) | (re & 0xffff)
            fsend[peer, first] = code.astype(jnp.int32)
        if group < len(PAIRS) - 1:
            slabs = [(first, first + 1 + 4 * count)]
        else:
            slabs = [(first + 1 + count * c - (c == 0), first + 1 + count * (c + 1)) for c in range(CHUNKS)]
        for start, stop in slabs:
            copies = []
            for n, (peer, peer_j) in enumerate(((cross, j), (i, j_next), (cross_mate, j), (mate, j_next), (mate, j),
                                                (cross, j_next), (cross_mate, j_next))):
                copy = pltpu.make_async_remote_copy(
                    src_ref=fsend.at[peer, start:stop], dst_ref=grecv.at[me, start:stop],
                    send_sem=a_send.at[len(a_copies), n], recv_sem=a_recv.at[len(a_copies), n],
                    device_id=(0, peer_j, peer), device_id_type=MESH)
                copy.start()
                copies.append(copy)
            a_copies.append(copies)
        stop = first + 1 + 4 * count
        grecv[me, first:stop] = fsend[i, first:stop]

    def unit_of(group):
        for src in range(8):
            scale[src, group] = jnp.exp(grecv[src, OFFSET[group]].astype(F32) * (1.0 / 1024.0)) * (1.0 / 32760.0)

    def first_stage(group, half, chunk):
        part = CHUNKS * half + chunk
        for b in GROUP_B[group]:
            values = []
            for a in range(8):
                src = 4 * half + a // 2
                tile, count = PLACE[8 * (a % 2) + b]
                word = grecv[src, tile + count * chunk]
                unit = scale[src, group]
                values.append((((word << 16) >> 16).astype(F32) * unit, (word >> 16).astype(F32) * unit))
            for c, value in enumerate(fft(values)):
                value = c_mul(value, b * c / 64)
                mid[part, c, b, 0] = value[0]
                mid[part, c, b, 1] = value[1]

    last = len(GROUP_B) - 1
    for group in range(last):
        for copy in a_copies[group]:
            copy.wait_recv()
        unit_of(group)

        def stage_part(part, carry):
            first_stage(group, part // CHUNKS, lax.rem(part, CHUNKS))
            return carry
        lax.fori_loop(0, 2 * CHUNKS, stage_part, 0)

    low_half = lax.broadcasted_iota(jnp.int32, (8, GRID), 1) < 64
    sign = (1 - 2 * j).astype(F32)
    loads[5].wait()
    loads[6].wait()

    def modes_of(chunk, total):
        for half in range(2):
            for c in range(8):
                values = fft([(mid[CHUNKS * half + chunk, c, b, 0], mid[CHUNKS * half + chunk, c, b, 1]) for b in range(8)])
                for d, value in enumerate(values):
                    k = c + 8 * d
                    turned = c_mul(value, k / 128)
                    left = jnp.where(low_half, value[0], pltpu.roll(value[1], 64, 1))
                    right = jnp.where(low_half, pltpu.roll(turned[0], 64, 1), turned[1])
                    hbuf[half, k] = left + sign * right
        rows = jnp.concatenate([hbuf[0].reshape(512, GRID), hbuf[1].reshape(512, GRID)], axis=1)
        high, low = split(rows)
        out = dot(high, z_table[0], NN) + dot(high, z_table[1], NN) + dot(low, z_table[0], NN)
        re, im = out[:, 0:GRID], out[:, GRID:]
        power = jnp.transpose((re * re + im * im).reshape(64, 8, GRID), (1, 0, 2))
        kx = pl.ds(8 * chunk, 8)
        mode = 0.5 * influence[kx] * power
        energy[kx] = mode
        return total + jnp.sum(mode.reshape(64, 8, GRID), axis=0)

    total = jnp.zeros((8, GRID), F32)
    for chunk in range(CHUNKS):
        for copy in a_copies[last + chunk]:
            copy.wait_recv()
        if chunk == 0:
            unit_of(last)
        for half in range(2):
            first_stage(last, half, chunk)
        total = modes_of(chunk, total)

    evec[...] = total
    e_copies = []
    for off in range(1, 8):
        peer = lax.rem(me + off, 8)
        copy = pltpu.make_async_remote_copy(
            src_ref=evec, dst_ref=erecv.at[me], send_sem=e_send.at[off], recv_sem=e_recv.at[off],
            device_id=(0, peer // 4, lax.rem(peer, 4)), device_id_type=MESH)
        copy.start()
        e_copies.append(copy)
    erecv[me] = total
    for copy in e_copies:
        copy.wait_recv()
    grand = erecv[0]
    for n in range(1, 8):
        grand = grand + erecv[n]
    total_out[0] = jnp.sum(grand) * (1.0 / (GRID * GRID * GRID))

    for copy in ghosts + [copy for copies in a_copies for copy in copies] + e_copies:
        copy.wait_send()


def solution(mesh):
    slot_spec = P(('sys', 'ydom', 'zdom'))
    mode_spec = P(('sys', 'ydom'), 'zdom', None)
    x_table, z_table = dft_tables()

    def local_energy(charge, real_mask, grid_idx, spline_w, influence):
        slots = charge.shape[0]
        blocks = slots // BLOCK
        hbm = pl.BlockSpec(memory_space=pltpu.HBM)
        groups = len(PAIRS)
        return pl.pallas_call(
            functools.partial(kernel, blocks),
            name='pme',
            out_shape=(jax.ShapeDtypeStruct(influence.shape, F32), jax.ShapeDtypeStruct((1,), F32)),
            in_specs=[hbm] * 7,
            out_specs=(pl.BlockSpec(memory_space=pltpu.VMEM), pl.BlockSpec(memory_space=pltpu.SMEM)),
            scratch_shapes=[
                pltpu.VMEM((1, slots), F32),
                pltpu.VMEM((1, slots), jnp.int32),
                pltpu.VMEM((3, slots), jnp.int32),
                pltpu.VMEM((3, 4, slots), F32),
                pltpu.VMEM(influence.shape, F32),
                pltpu.VMEM(x_table.shape, BF16),
                pltpu.VMEM(z_table.shape, BF16),
                pltpu.VMEM((blocks, 2 * GRID, BLOCK), BF16),
                pltpu.VMEM((blocks, Y_ROWS, BLOCK), F32),
                pltpu.VMEM((blocks, LEN_Z, BLOCK), F32),
                pltpu.VMEM((max(map(len, PAIRS)) * 2 * LEN_Z, GRID), F32),
                pltpu.VMEM((GHOST, LEN_Z, GRID), F32),
                pltpu.VMEM((GHOST, Y_ROWS, GRID), F32),
                pltpu.VMEM((GHOST, LEN_Z, GRID), F32),
                pltpu.VMEM((8 * LEN_Y, GRID), F32),
                pltpu.VMEM((8 * 8, GRID), F32),
                pltpu.VMEM((max(map(len, PAIRS)), 2 * GRID, GRID), F32),
                pltpu.VMEM((4, TILES, 8, GRID), jnp.int32),
                pltpu.VMEM((8, TILES, 8, GRID), jnp.int32),
                pltpu.VMEM((8, groups, 8, GRID), F32),
                pltpu.VMEM((2 * CHUNKS, 8, 8, 2, 8, GRID), F32),
                pltpu.VMEM((2, 64, 8, GRID), F32),
                pltpu.VMEM((8, GRID), F32),
                pltpu.VMEM((8, 8, GRID), F32),
                pltpu.SemaphoreType.DMA((7,)),
                pltpu.SemaphoreType.DMA((7,)),
                pltpu.SemaphoreType.DMA((7,)),
                pltpu.SemaphoreType.DMA((groups + CHUNKS - 1, 7)),
                pltpu.SemaphoreType.DMA((groups + CHUNKS - 1, 7)),
                pltpu.SemaphoreType.DMA((8,)),
                pltpu.SemaphoreType.DMA((8,)),
            ],
            compiler_params=pltpu.CompilerParams(collective_id=0, has_side_effects=True, vmem_limit_bytes=VMEM_LIMIT),
        )(*[pltpu.with_memory_space_constraint(value, pltpu.HBM) for value in (
            charge.reshape(1, slots), real_mask.reshape(1, slots), grid_idx.T,
            jnp.transpose(spline_w, (1, 2, 0)), influence, jnp.asarray(x_table), jnp.asarray(z_table))])

    return jax.shard_map(local_energy, mesh=mesh, in_specs=(slot_spec, slot_spec, P(('sys', 'ydom', 'zdom'), None), P(('sys', 'ydom', 'zdom'), None, None), mode_spec), out_specs=(mode_spec, P('sys')), check_vma=False)
```

```python
import functools
import math
import numpy as np
import jax
import jax.numpy as jnp
from jax import lax
from jax.experimental import pallas as pl
from jax.experimental.pallas import tpu as pltpu
from jax.sharding import PartitionSpec as P

MESH = pl.DeviceIdType.MESH
F32 = jnp.float32
BF16 = jnp.bfloat16
GRID = 128
LEN_Y = 32
LEN_Z = 64
GHOST = 3
BLOCK = 256
Y_ROWS = 40
CHUNKS = 4
UNROLL = 8
VMEM_LIMIT = 28 * 1024 * 1024
GROUP_B = ((2, 3), (4, 5), (0, 1), (6,), (7,))
PAIRS = tuple(tuple(bs) + tuple(8 + b for b in bs) for bs in GROUP_B)
OFFSET = tuple(sum(4 * len(p) + 1 for p in PAIRS[:g]) for g in range(len(PAIRS)))
TILES = sum(4 * len(p) + 1 for p in PAIRS)
PLACE = {pair: (OFFSET[g] + 1 + n, len(pairs)) for g, pairs in enumerate(PAIRS) for n, pair in enumerate(pairs)}
NT = (((1,), (1,)), ((), ()))
NN = (((1,), (0,)), ((), ()))


def split_table(table):
    table = np.asarray(table, np.float32)
    high = table.astype(jnp.bfloat16)
    low = (table - high.astype(np.float32)).astype(jnp.bfloat16)
    return np.stack([high, low])


def dft_tables():
    k = np.arange(GRID)
    phase = 2.0 * np.pi * ((k[:, None] * k[None, :]) % GRID) / GRID
    cos, sin = np.cos(phase), np.sin(phase)
    x_table = np.concatenate([cos, -sin], axis=0)
    z_table = []
    for half in range(2):
        c = cos[64 * half:64 * half + 64]
        s = sin[64 * half:64 * half + 64]
        z_table.append(np.block([[c, -s], [s, c]]))
    return split_table(x_table), split_table(np.concatenate(z_table, axis=0))


def split(value):
    high = value.astype(BF16)
    low = (value - high.astype(F32)).astype(BF16)
    return high, low


def dot(a, b, dims):
    return lax.dot_general(a, b, dims, preferred_element_type=F32)


def taps(base, weights, rows):
    delta = lax.broadcasted_iota(jnp.int32, (rows, base.shape[1]), 0) - base
    out = jnp.where(delta == 3, weights[3:4], 0.0)
    for s in (2, 1, 0):
        out = jnp.where(delta == s, weights[s:s + 1], out)
    return out


def c_add(a, b):
    return a[0] + b[0], a[1] + b[1]


def c_sub(a, b):
    return a[0] - b[0], a[1] - b[1]


def c_mul(a, turn):
    turn = turn % 1.0
    if turn == 0.0:
        return a
    if turn == 0.25:
        return a[1], -a[0]
    if turn == 0.5:
        return -a[0], -a[1]
    if turn == 0.75:
        return -a[1], a[0]
    c, s = math.cos(2 * math.pi * turn), math.sin(2 * math.pi * turn)
    if turn == 0.125:
        return c * (a[0] + a[1]), c * (a[1] - a[0])
    return c * a[0] + s * a[1], c * a[1] - s * a[0]


def fft(values):
    n = len(values)
    if n == 1:
        return values
    even, odd = fft(values[0::2]), fft(values[1::2])
    turned = [c_mul(o, k / n) for k, o in enumerate(odd)]
    return [c_add(e, t) for e, t in zip(even, turned)] + [c_sub(e, t) for e, t in zip(even, turned)]


def kernel(blocks, charge_hbm, mask_hbm, index_hbm, spline_hbm, influence_hbm, x_table_hbm, z_table_hbm,
           energy, total_out,
           charge, mask, index, spline, influence, x_table, z_table,
           xcat, yline, zline, acc, yghost, zghost, yface, zface, corner,
           modes, fsend, grecv, scale, mid, hbuf, evec, erecv,
           load_sem, ghost_send, ghost_recv, a_send, a_recv, e_send, e_recv):
    i = lax.axis_index('ydom')
    j = lax.axis_index('zdom')
    me = j * 4 + i
    i_next = lax.rem(i + 1, 4)
    j_next = 1 - j
    mate = i + 1 - 2 * lax.rem(i, 2)
    cross, cross_mate = lax.rem(i + 2, 4), lax.rem(mate + 2, 4)

    barrier = pltpu.get_barrier_semaphore()
    for off in range(1, 8):
        peer = lax.rem(me + off, 8)
        pl.semaphore_signal(barrier, inc=1, device_id=(0, peer // 4, lax.rem(peer, 4)), device_id_type=MESH)

    loads = [pltpu.make_async_copy(src, dst, load_sem.at[n]) for n, (src, dst) in enumerate(
        [(spline_hbm, spline), (index_hbm, index), (charge_hbm, charge), (mask_hbm, mask),
         (x_table_hbm, x_table), (z_table_hbm, z_table), (influence_hbm, influence)])]
    for copy in loads:
        copy.start()

    yghost[...] = jnp.zeros_like(yghost)
    zghost[...] = jnp.zeros_like(zghost)
    zface[GHOST * LEN_Y:] = jnp.zeros((5 * LEN_Y, GRID), F32)
    corner[GHOST * 8:] = jnp.zeros((5 * 8, GRID), F32)
    for copy in loads[:4]:
        copy.wait()

    def prepare(step, carry):
        total = None
        for n in range(4):
            b = 4 * step + n
            lanes = pl.ds(pl.multiple_of(b * BLOCK, BLOCK), BLOCK)
            weight = charge[:, lanes] * mask[:, lanes].astype(F32)
            wx = spline[0, :, lanes] * weight
            delta = (lax.broadcasted_iota(jnp.int32, (GRID, BLOCK), 0) - index[0:1, lanes]) & (GRID - 1)
            line = jnp.where(delta == 3, wx[3:4], 0.0)
            for s in (2, 1, 0):
                line = jnp.where(delta == s, wx[s:s + 1], line)
            cat = jnp.concatenate(split(line.T), axis=1)
            xcat[b] = cat
            yl = taps(index[1:2, lanes], spline[1, :, lanes], Y_ROWS)
            yline[b] = yl
            zl = taps(index[2:3, lanes], spline[2, :, lanes], LEN_Z + 8)
            zline[b] = zl[0:LEN_Z]
            rows = [yl[LEN_Y + t:LEN_Y + t + 1] * zl[0:LEN_Z] for t in range(GHOST)]
            rows += [zl[LEN_Z + u:LEN_Z + u + 1] * yl for u in range(GHOST)]
            rows += [jnp.zeros((8, BLOCK), F32)]
            high, low = split(jnp.concatenate(rows, axis=0))
            part = dot(high, cat, NN) + dot(low, cat, NN)
            total = part if total is None else total + part
        total = total[:, 0:GRID] + total[:, GRID:]
        yghost[...] += total[0:GHOST * LEN_Z].reshape(GHOST, LEN_Z, GRID)
        zghost[...] += total[GHOST * LEN_Z:GHOST * LEN_Z + GHOST * Y_ROWS].reshape(GHOST, Y_ROWS, GRID)
        return carry

    lax.fori_loop(0, blocks // 4, prepare, 0)

    pl.semaphore_wait(barrier, 7)
    ghosts = []
    for n, (src, dst, peer) in enumerate(
            [(yghost, yface, (0, j, i_next))]
            + [(zghost.at[u, 0:LEN_Y], zface.at[LEN_Y * u:LEN_Y * u + LEN_Y], (0, j_next, i)) for u in range(GHOST)]
            + [(zghost.at[u, LEN_Y:Y_ROWS], corner.at[8 * u:8 * u + 8], (0, j_next, i_next)) for u in range(GHOST)]):
        copy = pltpu.make_async_remote_copy(
            src_ref=src, dst_ref=dst, send_sem=ghost_send.at[n], recv_sem=ghost_recv.at[n],
            device_id=peer, device_id_type=MESH)
        copy.start()
        ghosts.append(copy)

    def spread_rows(pairs):
        count = 2 * LEN_Z * len(pairs)
        acc[0:count] = jnp.zeros((count, GRID), F32)

        def body(step, carry):
            both = None
            for n in range(UNROLL):
                b = UNROLL * step + n
                zl = zline[b]
                high, low = split(jnp.concatenate(
                    [yline[b, 2 * pair + h:2 * pair + h + 1] * zl for pair in pairs for h in range(2)], axis=0))
                part = dot(high, xcat[b], NN) + dot(low, xcat[b], NN)
                both = part if both is None else both + part
            acc[0:count] += both[:, 0:GRID] + both[:, GRID:]
            return carry
        lax.fori_loop(0, blocks // UNROLL, body, 0)

    a_copies = []
    for group, pairs in enumerate(PAIRS):
        spread_rows(pairs)
        if group == 0:
            for copy in ghosts:
                copy.wait_recv()
            loads[4].wait()
        for n, pair in enumerate(pairs):
            for h in range(2):
                y, row = 2 * pair + h, 64 * (2 * n + h)
                if y < GHOST:
                    acc[row:row + LEN_Z] += yface[y]
                    acc[row:row + 8] += corner[pl.ds(y, 8, stride=8)]
                acc[row:row + 8] += zface[pl.ds(y, 8, stride=LEN_Y)]
        for n in range(len(pairs)):
            high, low = split(acc[128 * n:128 * n + 128])
            modes[n] = dot(x_table[0], high, NT) + dot(x_table[1], high, NT) + dot(x_table[0], low, NT)
        first, count = OFFSET[group], len(pairs)
        for peer in range(4):
            at = [(n, c, 32 * peer + 8 * c) for n in range(len(pairs)) for c in range(CHUNKS)]
            top = jnp.full((8, GRID), 1e-30, F32)
            for n, c, row in at:
                top = jnp.maximum(top, jnp.maximum(jnp.abs(modes[n, row:row + 8]), jnp.abs(modes[n, GRID + row:GRID + row + 8])))
            code = jnp.ceil(jnp.log(top) * 1024.0)
            inverse = 32760.0 / jnp.exp(code * (1.0 / 1024.0))
            for n, c, row in at:
                re = jnp.round(modes[n, row:row + 8] * inverse).astype(jnp.int32)
                im = jnp.round(modes[n, GRID + row:GRID + row + 8] * inverse).astype(jnp.int32)
                fsend[peer, first + 1 + count * c + n] = (im << 16) | (re & 0xffff)
            fsend[peer, first] = code.astype(jnp.int32)
        if group < len(PAIRS) - 1:
            slabs = [(first, first + 1 + 4 * count)]
        else:
            slabs = [(first, first + 1 + 2 * count), (first + 1 + 2 * count, first + 1 + 4 * count)]
        for start, stop in slabs:
            copies = []
            for n, (peer, peer_j) in enumerate(((cross, j), (i, j_next), (cross_mate, j), (mate, j_next), (mate, j),
                                                (cross, j_next), (cross_mate, j_next))):
                copy = pltpu.make_async_remote_copy(
                    src_ref=fsend.at[peer, start:stop], dst_ref=grecv.at[me, start:stop],
                    send_sem=a_send.at[len(a_copies), n], recv_sem=a_recv.at[len(a_copies), n],
                    device_id=(0, peer_j, peer), device_id_type=MESH)
                copy.start()
                copies.append(copy)
            a_copies.append(copies)
        stop = first + 1 + 4 * count
        grecv[me, first:stop] = fsend[i, first:stop]

    def unit_of(group):
        for src in range(8):
            scale[src, group] = jnp.exp(grecv[src, OFFSET[group]].astype(F32) * (1.0 / 1024.0)) * (1.0 / 32760.0)

    def first_stage(group, half, chunk):
        part = CHUNKS * half + chunk
        for b in GROUP_B[group]:
            values = []
            for a in range(8):
                src = 4 * half + a // 2
                tile, count = PLACE[8 * (a % 2) + b]
                word = grecv[src, tile + count * chunk]
                unit = scale[src, group]
                values.append((((word << 16) >> 16).astype(F32) * unit, (word >> 16).astype(F32) * unit))
            for c, value in enumerate(fft(values)):
                value = c_mul(value, b * c / 64)
                mid[part, c, b, 0] = value[0]
                mid[part, c, b, 1] = value[1]

    last = len(GROUP_B) - 1
    for group in range(last):
        for copy in a_copies[group]:
            copy.wait_recv()
        unit_of(group)

        def stage_part(part, carry):
            first_stage(group, part // CHUNKS, lax.rem(part, CHUNKS))
            return carry
        lax.fori_loop(0, 2 * CHUNKS, stage_part, 0)

    low_half = lax.broadcasted_iota(jnp.int32, (8, GRID), 1) < 64
    sign = (1 - 2 * j).astype(F32)
    loads[5].wait()
    loads[6].wait()

    def modes_of(chunk, total):
        for half in range(2):
            for c in range(8):
                values = fft([(mid[CHUNKS * half + chunk, c, b, 0], mid[CHUNKS * half + chunk, c, b, 1]) for b in range(8)])
                for d, value in enumerate(values):
                    k = c + 8 * d
                    turned = c_mul(value, k / 128)
                    left = jnp.where(low_half, value[0], pltpu.roll(value[1], 64, 1))
                    right = jnp.where(low_half, pltpu.roll(turned[0], 64, 1), turned[1])
                    hbuf[half, k] = left + sign * right
        rows = jnp.concatenate([hbuf[0].reshape(512, GRID), hbuf[1].reshape(512, GRID)], axis=1)
        high, low = split(rows)
        out = dot(high, z_table[0], NN) + dot(high, z_table[1], NN) + dot(low, z_table[0], NN)
        re, im = out[:, 0:GRID], out[:, GRID:]
        power = jnp.transpose((re * re + im * im).reshape(64, 8, GRID), (1, 0, 2))
        kx = pl.ds(8 * chunk, 8)
        mode = 0.5 * influence[kx] * power
        energy[kx] = mode
        return total + jnp.sum(mode.reshape(64, 8, GRID), axis=0)

    total = jnp.zeros((8, GRID), F32)
    for chunk in range(CHUNKS):
        if chunk % 2 == 0:
            for copy in a_copies[last + chunk // 2]:
                copy.wait_recv()
        if chunk == 0:
            unit_of(last)
        for half in range(2):
            first_stage(last, half, chunk)
        total = modes_of(chunk, total)

    evec[...] = total
    e_copies = []
    for off in range(1, 8):
        peer = lax.rem(me + off, 8)
        copy = pltpu.make_async_remote_copy(
            src_ref=evec, dst_ref=erecv.at[me], send_sem=e_send.at[off], recv_sem=e_recv.at[off],
            device_id=(0, peer // 4, lax.rem(peer, 4)), device_id_type=MESH)
        copy.start()
        e_copies.append(copy)
    erecv[me] = total
    for copy in e_copies:
        copy.wait_recv()
    grand = erecv[0]
    for n in range(1, 8):
        grand = grand + erecv[n]
    total_out[0] = jnp.sum(grand) * (1.0 / (GRID * GRID * GRID))

    for copy in ghosts + [copy for copies in a_copies for copy in copies] + e_copies:
        copy.wait_send()


def solution(mesh):
    slot_spec = P(('sys', 'ydom', 'zdom'))
    mode_spec = P(('sys', 'ydom'), 'zdom', None)
    x_table, z_table = dft_tables()

    def local_energy(charge, real_mask, grid_idx, spline_w, influence):
        slots = charge.shape[0]
        blocks = slots // BLOCK
        hbm = pl.BlockSpec(memory_space=pltpu.HBM)
        groups = len(PAIRS)
        return pl.pallas_call(
            functools.partial(kernel, blocks),
            name='pme',
            out_shape=(jax.ShapeDtypeStruct(influence.shape, F32), jax.ShapeDtypeStruct((1,), F32)),
            in_specs=[hbm] * 7,
            out_specs=(pl.BlockSpec(memory_space=pltpu.VMEM), pl.BlockSpec(memory_space=pltpu.SMEM)),
            scratch_shapes=[
                pltpu.VMEM((1, slots), F32),
                pltpu.VMEM((1, slots), jnp.int32),
                pltpu.VMEM((3, slots), jnp.int32),
                pltpu.VMEM((3, 4, slots), F32),
                pltpu.VMEM(influence.shape, F32),
                pltpu.VMEM(x_table.shape, BF16),
                pltpu.VMEM(z_table.shape, BF16),
                pltpu.VMEM((blocks, BLOCK, 2 * GRID), BF16),
                pltpu.VMEM((blocks, Y_ROWS, BLOCK), F32),
                pltpu.VMEM((blocks, LEN_Z, BLOCK), F32),
                pltpu.VMEM((max(map(len, PAIRS)) * 2 * LEN_Z, GRID), F32),
                pltpu.VMEM((GHOST, LEN_Z, GRID), F32),
                pltpu.VMEM((GHOST, Y_ROWS, GRID), F32),
                pltpu.VMEM((GHOST, LEN_Z, GRID), F32),
                pltpu.VMEM((8 * LEN_Y, GRID), F32),
                pltpu.VMEM((8 * 8, GRID), F32),
                pltpu.VMEM((max(map(len, PAIRS)), 2 * GRID, GRID), F32),
                pltpu.VMEM((4, TILES, 8, GRID), jnp.int32),
                pltpu.VMEM((8, TILES, 8, GRID), jnp.int32),
                pltpu.VMEM((8, groups, 8, GRID), F32),
                pltpu.VMEM((2 * CHUNKS, 8, 8, 2, 8, GRID), F32),
                pltpu.VMEM((2, 64, 8, GRID), F32),
                pltpu.VMEM((8, GRID), F32),
                pltpu.VMEM((8, 8, GRID), F32),
                pltpu.SemaphoreType.DMA((7,)),
                pltpu.SemaphoreType.DMA((7,)),
                pltpu.SemaphoreType.DMA((7,)),
                pltpu.SemaphoreType.DMA((groups + 1, 7)),
                pltpu.SemaphoreType.DMA((groups + 1, 7)),
                pltpu.SemaphoreType.DMA((8,)),
                pltpu.SemaphoreType.DMA((8,)),
            ],
            compiler_params=pltpu.CompilerParams(collective_id=0, has_side_effects=True, vmem_limit_bytes=VMEM_LIMIT),
        )(*[pltpu.with_memory_space_constraint(value, pltpu.HBM) for value in (
            charge.reshape(1, slots), real_mask.reshape(1, slots), grid_idx.T,
            jnp.transpose(spline_w, (1, 2, 0)), influence, jnp.asarray(x_table), jnp.asarray(z_table))])

    return jax.shard_map(local_energy, mesh=mesh, in_specs=(slot_spec, slot_spec, P(('sys', 'ydom', 'zdom'), None), P(('sys', 'ydom', 'zdom'), None, None), mode_spec), out_specs=(mode_spec, P('sys')), check_vma=False)
```

```python
import functools
import math
import numpy as np
import jax
import jax.numpy as jnp
from jax import lax
from jax.experimental import pallas as pl
from jax.experimental.pallas import tpu as pltpu
from jax.sharding import PartitionSpec as P

MESH = pl.DeviceIdType.MESH
F32 = jnp.float32
BF16 = jnp.bfloat16
GRID = 128
LEN_Y = 32
LEN_Z = 64
GHOST = 3
BLOCK = 256
Y_ROWS = 40
CHUNKS = 4
UNROLL = 16
VMEM_LIMIT = 28 * 1024 * 1024
GROUP_B = ((2, 3), (4, 5), (0, 1), (6,), (7,))
PAIRS = tuple(tuple(bs) + tuple(8 + b for b in bs) for bs in GROUP_B)
OFFSET = tuple(sum(4 * len(p) + 1 for p in PAIRS[:g]) for g in range(len(PAIRS)))
TILES = sum(4 * len(p) + 1 for p in PAIRS)
PLACE = {pair: (OFFSET[g] + 1 + n, len(pairs)) for g, pairs in enumerate(PAIRS) for n, pair in enumerate(pairs)}
NT = (((1,), (1,)), ((), ()))
NN = (((1,), (0,)), ((), ()))


def split_table(table):
    table = np.asarray(table, np.float32)
    high = table.astype(jnp.bfloat16)
    low = (table - high.astype(np.float32)).astype(jnp.bfloat16)
    return np.stack([high, low])


def dft_tables():
    k = np.arange(GRID)
    phase = 2.0 * np.pi * ((k[:, None] * k[None, :]) % GRID) / GRID
    cos, sin = np.cos(phase), np.sin(phase)
    x_table = np.concatenate([cos, -sin], axis=0)
    z_table = []
    for half in range(2):
        c = cos[64 * half:64 * half + 64]
        s = sin[64 * half:64 * half + 64]
        z_table.append(np.block([[c, -s], [s, c]]))
    return split_table(x_table), split_table(np.concatenate(z_table, axis=0))


def split(value):
    high = value.astype(BF16)
    low = (value - high.astype(F32)).astype(BF16)
    return high, low


def dot(a, b, dims):
    return lax.dot_general(a, b, dims, preferred_element_type=F32)


def taps(base, weights, rows):
    delta = lax.broadcasted_iota(jnp.int32, (rows, base.shape[1]), 0) - base
    out = jnp.where(delta == 3, weights[3:4], 0.0)
    for s in (2, 1, 0):
        out = jnp.where(delta == s, weights[s:s + 1], out)
    return out


def c_add(a, b):
    return a[0] + b[0], a[1] + b[1]


def c_sub(a, b):
    return a[0] - b[0], a[1] - b[1]


def c_mul(a, turn):
    turn = turn % 1.0
    if turn == 0.0:
        return a
    if turn == 0.25:
        return a[1], -a[0]
    if turn == 0.5:
        return -a[0], -a[1]
    if turn == 0.75:
        return -a[1], a[0]
    c, s = math.cos(2 * math.pi * turn), math.sin(2 * math.pi * turn)
    if turn == 0.125:
        return c * (a[0] + a[1]), c * (a[1] - a[0])
    return c * a[0] + s * a[1], c * a[1] - s * a[0]


def fft(values):
    n = len(values)
    if n == 1:
        return values
    even, odd = fft(values[0::2]), fft(values[1::2])
    turned = [c_mul(o, k / n) for k, o in enumerate(odd)]
    return [c_add(e, t) for e, t in zip(even, turned)] + [c_sub(e, t) for e, t in zip(even, turned)]


def kernel(blocks, charge_hbm, mask_hbm, index_hbm, spline_hbm, influence_hbm, x_table_hbm, z_table_hbm,
           energy, total_out,
           charge, mask, index, spline, influence, x_table, z_table,
           xcat, yline, zline, acc, yghost, zghost, yface, zface, corner,
           modes, fsend, grecv, scale, mid, hbuf, evec, erecv,
           load_sem, ghost_send, ghost_recv, a_send, a_recv, e_send, e_recv):
    i = lax.axis_index('ydom')
    j = lax.axis_index('zdom')
    me = j * 4 + i
    i_next = lax.rem(i + 1, 4)
    j_next = 1 - j
    mate = i + 1 - 2 * lax.rem(i, 2)
    cross, cross_mate = lax.rem(i + 2, 4), lax.rem(mate + 2, 4)

    barrier = pltpu.get_barrier_semaphore()
    for off in range(1, 8):
        peer = lax.rem(me + off, 8)
        pl.semaphore_signal(barrier, inc=1, device_id=(0, peer // 4, lax.rem(peer, 4)), device_id_type=MESH)

    loads = [pltpu.make_async_copy(src, dst, load_sem.at[n]) for n, (src, dst) in enumerate(
        [(spline_hbm, spline), (index_hbm, index), (charge_hbm, charge), (mask_hbm, mask),
         (x_table_hbm, x_table), (z_table_hbm, z_table), (influence_hbm, influence)])]
    for copy in loads:
        copy.start()

    yghost[...] = jnp.zeros_like(yghost)
    zghost[...] = jnp.zeros_like(zghost)
    zface[GHOST * LEN_Y:] = jnp.zeros((5 * LEN_Y, GRID), F32)
    corner[GHOST * 8:] = jnp.zeros((5 * 8, GRID), F32)
    for copy in loads[:4]:
        copy.wait()

    def prepare(step, carry):
        total = None
        for n in range(4):
            b = 4 * step + n
            lanes = pl.ds(pl.multiple_of(b * BLOCK, BLOCK), BLOCK)
            weight = charge[:, lanes] * mask[:, lanes].astype(F32)
            wx = spline[0, :, lanes] * weight
            delta = (lax.broadcasted_iota(jnp.int32, (GRID, BLOCK), 0) - index[0:1, lanes]) & (GRID - 1)
            line = jnp.where(delta == 3, wx[3:4], 0.0)
            for s in (2, 1, 0):
                line = jnp.where(delta == s, wx[s:s + 1], line)
            cat = jnp.concatenate(split(line.T), axis=1)
            xcat[b] = cat
            yl = taps(index[1:2, lanes], spline[1, :, lanes], Y_ROWS)
            yline[b] = yl
            zl = taps(index[2:3, lanes], spline[2, :, lanes], LEN_Z + 8)
            zline[b] = zl[0:LEN_Z]
            rows = [yl[LEN_Y + t:LEN_Y + t + 1] * zl[0:LEN_Z] for t in range(GHOST)]
            rows += [zl[LEN_Z + u:LEN_Z + u + 1] * yl for u in range(GHOST)]
            rows += [jnp.zeros((8, BLOCK), F32)]
            high, low = split(jnp.concatenate(rows, axis=0))
            part = dot(high, cat, NN) + dot(low, cat, NN)
            total = part if total is None else total + part
        total = total[:, 0:GRID] + total[:, GRID:]
        yghost[...] += total[0:GHOST * LEN_Z].reshape(GHOST, LEN_Z, GRID)
        zghost[...] += total[GHOST * LEN_Z:GHOST * LEN_Z + GHOST * Y_ROWS].reshape(GHOST, Y_ROWS, GRID)
        return carry

    lax.fori_loop(0, blocks // 4, prepare, 0)

    pl.semaphore_wait(barrier, 7)
    ghosts = []
    for n, (src, dst, peer) in enumerate(
            [(yghost, yface, (0, j, i_next))]
            + [(zghost.at[u, 0:LEN_Y], zface.at[LEN_Y * u:LEN_Y * u + LEN_Y], (0, j_next, i)) for u in range(GHOST)]
            + [(zghost.at[u, LEN_Y:Y_ROWS], corner.at[8 * u:8 * u + 8], (0, j_next, i_next)) for u in range(GHOST)]):
        copy = pltpu.make_async_remote_copy(
            src_ref=src, dst_ref=dst, send_sem=ghost_send.at[n], recv_sem=ghost_recv.at[n],
            device_id=peer, device_id_type=MESH)
        copy.start()
        ghosts.append(copy)

    def spread_rows(pairs):
        count = 2 * LEN_Z * len(pairs)
        acc[0:count] = jnp.zeros((count, GRID), F32)

        def body(step, carry):
            both = None
            for n in range(UNROLL):
                b = UNROLL * step + n
                zl = zline[b]
                high, low = split(jnp.concatenate(
                    [yline[b, 2 * pair + h:2 * pair + h + 1] * zl for pair in pairs for h in range(2)], axis=0))
                part = dot(high, xcat[b], NN) + dot(low, xcat[b], NN)
                both = part if both is None else both + part
            acc[0:count] += both[:, 0:GRID] + both[:, GRID:]
            return carry
        lax.fori_loop(0, blocks // UNROLL, body, 0)

    a_copies = []
    for group, pairs in enumerate(PAIRS):
        spread_rows(pairs)
        if group == 0:
            for copy in ghosts:
                copy.wait_recv()
            loads[4].wait()
        for n, pair in enumerate(pairs):
            for h in range(2):
                y, row = 2 * pair + h, 64 * (2 * n + h)
                if y < GHOST:
                    acc[row:row + LEN_Z] += yface[y]
                    acc[row:row + 8] += corner[pl.ds(y, 8, stride=8)]
                acc[row:row + 8] += zface[pl.ds(y, 8, stride=LEN_Y)]
        for n in range(len(pairs)):
            high, low = split(acc[128 * n:128 * n + 128])
            modes[n] = dot(x_table[0], high, NT) + dot(x_table[1], high, NT) + dot(x_table[0], low, NT)
        first, count = OFFSET[group], len(pairs)
        for peer in range(4):
            at = [(n, c, 32 * peer + 8 * c) for n in range(len(pairs)) for c in range(CHUNKS)]
            top = jnp.full((8, GRID), 1e-30, F32)
            for n, c, row in at:
                top = jnp.maximum(top, jnp.maximum(jnp.abs(modes[n, row:row + 8]), jnp.abs(modes[n, GRID + row:GRID + row + 8])))
            code = jnp.ceil(jnp.log(top) * 1024.0)
            inverse = 32760.0 / jnp.exp(code * (1.0 / 1024.0))
            for n, c, row in at:
                re = jnp.round(modes[n, row:row + 8] * inverse).astype(jnp.int32)
                im = jnp.round(modes[n, GRID + row:GRID + row + 8] * inverse).astype(jnp.int32)
                fsend[peer, first + 1 + count * c + n] = (im << 16) | (re & 0xffff)
            fsend[peer, first] = code.astype(jnp.int32)
        if group < len(PAIRS) - 1:
            slabs = [(first, first + 1 + 4 * count)]
        else:
            slabs = [(first, first + 1 + 2 * count), (first + 1 + 2 * count, first + 1 + 4 * count)]
        for start, stop in slabs:
            copies = []
            for n, (peer, peer_j) in enumerate(((cross, j), (i, j_next), (cross_mate, j), (mate, j_next), (mate, j),
                                                (cross, j_next), (cross_mate, j_next))):
                copy = pltpu.make_async_remote_copy(
                    src_ref=fsend.at[peer, start:stop], dst_ref=grecv.at[me, start:stop],
                    send_sem=a_send.at[len(a_copies), n], recv_sem=a_recv.at[len(a_copies), n],
                    device_id=(0, peer_j, peer), device_id_type=MESH)
                copy.start()
                copies.append(copy)
            a_copies.append(copies)
        stop = first + 1 + 4 * count
        grecv[me, first:stop] = fsend[i, first:stop]

    def unit_of(group):
        for src in range(8):
            scale[src, group] = jnp.exp(grecv[src, OFFSET[group]].astype(F32) * (1.0 / 1024.0)) * (1.0 / 32760.0)

    def first_stage(group, half, chunk):
        part = CHUNKS * half + chunk
        for b in GROUP_B[group]:
            values = []
            for a in range(8):
                src = 4 * half + a // 2
                tile, count = PLACE[8 * (a % 2) + b]
                word = grecv[src, tile + count * chunk]
                unit = scale[src, group]
                values.append((((word << 16) >> 16).astype(F32) * unit, (word >> 16).astype(F32) * unit))
            for c, value in enumerate(fft(values)):
                value = c_mul(value, b * c / 64)
                mid[part, c, b, 0] = value[0]
                mid[part, c, b, 1] = value[1]

    last = len(GROUP_B) - 1
    for group in range(last):
        for copy in a_copies[group]:
            copy.wait_recv()
        unit_of(group)

        def stage_part(part, carry):
            first_stage(group, part // CHUNKS, lax.rem(part, CHUNKS))
            return carry
        lax.fori_loop(0, 2 * CHUNKS, stage_part, 0)

    low_half = lax.broadcasted_iota(jnp.int32, (8, GRID), 1) < 64
    sign = (1 - 2 * j).astype(F32)
    loads[5].wait()
    loads[6].wait()

    def modes_of(chunk, total):
        for half in range(2):
            for c in range(8):
                values = fft([(mid[CHUNKS * half + chunk, c, b, 0], mid[CHUNKS * half + chunk, c, b, 1]) for b in range(8)])
                for d, value in enumerate(values):
                    k = c + 8 * d
                    turned = c_mul(value, k / 128)
                    left = jnp.where(low_half, value[0], pltpu.roll(value[1], 64, 1))
                    right = jnp.where(low_half, pltpu.roll(turned[0], 64, 1), turned[1])
                    hbuf[half, k] = left + sign * right
        rows = jnp.concatenate([hbuf[0].reshape(512, GRID), hbuf[1].reshape(512, GRID)], axis=1)
        high, low = split(rows)
        out = dot(high, z_table[0], NN) + dot(high, z_table[1], NN) + dot(low, z_table[0], NN)
        re, im = out[:, 0:GRID], out[:, GRID:]
        power = jnp.transpose((re * re + im * im).reshape(64, 8, GRID), (1, 0, 2))
        kx = pl.ds(8 * chunk, 8)
        mode = 0.5 * influence[kx] * power
        energy[kx] = mode
        return total + jnp.sum(mode.reshape(64, 8, GRID), axis=0)

    total = jnp.zeros((8, GRID), F32)
    for chunk in range(CHUNKS):
        if chunk % 2 == 0:
            for copy in a_copies[last + chunk // 2]:
                copy.wait_recv()
        if chunk == 0:
            unit_of(last)
        for half in range(2):
            first_stage(last, half, chunk)
        total = modes_of(chunk, total)

    evec[...] = total
    e_copies = []
    for off in range(1, 8):
        peer = lax.rem(me + off, 8)
        copy = pltpu.make_async_remote_copy(
            src_ref=evec, dst_ref=erecv.at[me], send_sem=e_send.at[off], recv_sem=e_recv.at[off],
            device_id=(0, peer // 4, lax.rem(peer, 4)), device_id_type=MESH)
        copy.start()
        e_copies.append(copy)
    erecv[me] = total
    for copy in e_copies:
        copy.wait_recv()
    grand = erecv[0]
    for n in range(1, 8):
        grand = grand + erecv[n]
    total_out[0] = jnp.sum(grand) * (1.0 / (GRID * GRID * GRID))

    for copy in ghosts + [copy for copies in a_copies for copy in copies] + e_copies:
        copy.wait_send()


def solution(mesh):
    slot_spec = P(('sys', 'ydom', 'zdom'))
    mode_spec = P(('sys', 'ydom'), 'zdom', None)
    x_table, z_table = dft_tables()

    def local_energy(charge, real_mask, grid_idx, spline_w, influence):
        slots = charge.shape[0]
        blocks = slots // BLOCK
        hbm = pl.BlockSpec(memory_space=pltpu.HBM)
        groups = len(PAIRS)
        return pl.pallas_call(
            functools.partial(kernel, blocks),
            name='pme',
            out_shape=(jax.ShapeDtypeStruct(influence.shape, F32), jax.ShapeDtypeStruct((1,), F32)),
            in_specs=[hbm] * 7,
            out_specs=(pl.BlockSpec(memory_space=pltpu.VMEM), pl.BlockSpec(memory_space=pltpu.SMEM)),
            scratch_shapes=[
                pltpu.VMEM((1, slots), F32),
                pltpu.VMEM((1, slots), jnp.int32),
                pltpu.VMEM((3, slots), jnp.int32),
                pltpu.VMEM((3, 4, slots), F32),
                pltpu.VMEM(influence.shape, F32),
                pltpu.VMEM(x_table.shape, BF16),
                pltpu.VMEM(z_table.shape, BF16),
                pltpu.VMEM((blocks, BLOCK, 2 * GRID), BF16),
                pltpu.VMEM((blocks, Y_ROWS, BLOCK), F32),
                pltpu.VMEM((blocks, LEN_Z, BLOCK), F32),
                pltpu.VMEM((max(map(len, PAIRS)) * 2 * LEN_Z, GRID), F32),
                pltpu.VMEM((GHOST, LEN_Z, GRID), F32),
                pltpu.VMEM((GHOST, Y_ROWS, GRID), F32),
                pltpu.VMEM((GHOST, LEN_Z, GRID), F32),
                pltpu.VMEM((8 * LEN_Y, GRID), F32),
                pltpu.VMEM((8 * 8, GRID), F32),
                pltpu.VMEM((max(map(len, PAIRS)), 2 * GRID, GRID), F32),
                pltpu.VMEM((4, TILES, 8, GRID), jnp.int32),
                pltpu.VMEM((8, TILES, 8, GRID), jnp.int32),
                pltpu.VMEM((8, groups, 8, GRID), F32),
                pltpu.VMEM((2 * CHUNKS, 8, 8, 2, 8, GRID), F32),
                pltpu.VMEM((2, 64, 8, GRID), F32),
                pltpu.VMEM((8, GRID), F32),
                pltpu.VMEM((8, 8, GRID), F32),
                pltpu.SemaphoreType.DMA((7,)),
                pltpu.SemaphoreType.DMA((7,)),
                pltpu.SemaphoreType.DMA((7,)),
                pltpu.SemaphoreType.DMA((groups + 1, 7)),
                pltpu.SemaphoreType.DMA((groups + 1, 7)),
                pltpu.SemaphoreType.DMA((8,)),
                pltpu.SemaphoreType.DMA((8,)),
            ],
            compiler_params=pltpu.CompilerParams(collective_id=0, has_side_effects=True, vmem_limit_bytes=VMEM_LIMIT),
        )(*[pltpu.with_memory_space_constraint(value, pltpu.HBM) for value in (
            charge.reshape(1, slots), real_mask.reshape(1, slots), grid_idx.T,
            jnp.transpose(spline_w, (1, 2, 0)), influence, jnp.asarray(x_table), jnp.asarray(z_table))])

    return jax.shard_map(local_energy, mesh=mesh, in_specs=(slot_spec, slot_spec, P(('sys', 'ydom', 'zdom'), None), P(('sys', 'ydom', 'zdom'), None, None), mode_spec), out_specs=(mode_spec, P('sys')), check_vma=False)
```
